128 devices in a mesh: row: 8 (over x, core), col: 16 (over y, z).
Axes of the slice: x: 4, y: 4, z: 4, core: 2. Of those that a mesh axis runs over, the one named last changes fastest.
Arguments:
- points: float32 [16, 32768], P(None, ('row', 'col')), may hold values from -6 to 6
- lengthscale: float32 [16], replicated, may hold values from 2 to 8
- signal: float32 [1], replicated, may hold values from 0.5 to 2
- noise: float32 [1], replicated, may hold values from 0.05 to 0.5
- targets: float32 [32768], P(('row', 'col')), may hold values from -12 to 12
- probe_bits: int32 [31, 32768], P(None, ('row', 'col')), may hold values from 0 to 1
Outputs:
- solution: float32 [32, 32768], P(None, ('row', 'col'))
- residual: float32 [32, 32768], P(None, ('row', 'col'))
The draws below stay inside these ranges and needn't reach their ends.
All inputs are finite; a program needn't handle non-finite values.
Results may differ from the reference program's by a relative error of at most 0.0013.
Values sent between devices are 32-bit elements; how exact they have to be, the bound alone decides.
A program may use at most 128 MiB of HBM per device.

```python
import math
import jax
import jax.numpy as jnp
from jax import lax

DIM = 16
PROBES = 31
ITERS = 3
N = 32768


def draw_targets(key, part):
    ramp = 1.0 + 2.0 * jnp.arange(N, dtype=jnp.float32) / N
    values = jnp.clip(jax.random.normal(key, (N,), jnp.float32), -4.0, 4.0)
    return values * ramp


def with_ends(array, stream_key, least, high):
    index_at = [jax.random.randint(jax.random.fold_in(stream_key, axis), (), 0, length) for axis, length in enumerate(array.shape)]
    longest = array.shape.index(max(array.shape))
    next_to = index_at[:longest] + [(index_at[longest] + 1) % array.shape[longest]] + index_at[longest + 1:]
    return array.at[tuple(index_at)].set(least).at[tuple(next_to)].set(high)


def level_of(stream_key, extent, split, low, high):
    def one(position, parts):
        draws = jax.random.uniform(jax.random.fold_in(jax.random.fold_in(stream_key, 6), position), (parts,), jnp.float32, low / len(split), high / len(split))
        return jnp.repeat(jnp.exp(draws), extent[position] // parts).reshape((-1,) + (1,) * (len(extent) - position - 1))

    factor_of = one(*split[0])
    for cut in split[1:]:
        factor_of = factor_of * one(*cut)
    return factor_of


def gaussian(stream_key, dims, spread, most, cuts=(), kind=jnp.bfloat16):
    values = jax.random.normal(stream_key, dims, jnp.float32) * spread
    if len(cuts) > 0:
        values = level_of(stream_key, dims, cuts, -0.22, 0.18) * values
    return jnp.clip(values, min=-most, max=most).astype(kind)


def setup_inputs(seed: int = 0) -> dict:
    keys = jax.random.split(jax.random.key(seed), 7)
    return {
        "points": gaussian(keys[0], (DIM, N), 1.0, 6.0, ((1, 128),), jnp.float32),
        "lengthscale": jnp.clip(jnp.exp(jax.random.uniform(keys[1], (DIM,), jnp.float32, math.log(2.0), math.log(8.0))), 2.0, 8.0),
        "signal": jnp.clip(jnp.exp(jax.random.uniform(keys[2], (1,), jnp.float32, math.log(0.5), math.log(2.0))), 0.5, 2.0),
        "noise": jnp.clip(jnp.exp(jax.random.uniform(keys[3], (1,), jnp.float32, math.log(0.05), math.log(0.5))), 0.05, 0.5),
        "targets": draw_targets(jax.random.fold_in(keys[6], 71), 0),
        "probe_bits": with_ends(jax.random.randint(keys[5], (PROBES, N), 0, 2), jax.random.fold_in(keys[5], 1), 0, 1).astype(jnp.int32),
    }


ROOT_FIVE = 5.0 ** 0.5

def matern_tile(row_scaled, col_scaled, signal_value):
    row_sq = lax.optimization_barrier(jnp.sum(row_scaled * row_scaled, axis=0))
    col_sq = lax.optimization_barrier(jnp.sum(col_scaled * col_scaled, axis=0))
    cross_term = lax.dot_general(row_scaled, col_scaled, (((0,), (0,)), ((), ())), precision=lax.Precision.HIGHEST, preferred_element_type=jnp.float32)
    dist_sq = jnp.maximum(row_sq[:, None] + col_sq[None, :] - 2.0 * cross_term, 0.0)
    radius = jnp.sqrt(dist_sq)
    return signal_value * (1.0 + ROOT_FIVE * radius + 5.0 / 3.0 * dist_sq) * jnp.exp(-ROOT_FIVE * radius)

def reference(points, lengthscale, signal, noise, targets, probe_bits):
    scaled = points / lengthscale[:, None]
    signs = 2.0 * probe_bits.astype(jnp.float32) - 1.0
    right_side = jnp.concatenate([targets[None, :], signs], axis=0)
    signal_value = signal[0]
    noise_value = noise[0]
    block_rows = min(2048, N)
    stacked = scaled.reshape(DIM, N // block_rows, block_rows).transpose(1, 0, 2)

    def operator(vectors):

        def one_block(row_block):
            kernel_tile = matern_tile(row_block, scaled, signal_value)
            return lax.dot_general(vectors, kernel_tile, (((1,), (1,)), ((), ())), precision=lax.Precision.HIGHEST, preferred_element_type=jnp.float32)
        pieces = lax.map(one_block, stacked)
        return pieces.transpose(1, 0, 2).reshape(vectors.shape[0], N) + noise_value * vectors
    solution = jnp.zeros_like(right_side)
    residual = right_side
    direction = right_side
    norm_now = lax.optimization_barrier(jnp.sum(residual * residual, axis=1))
    for step in range(ITERS):
        image = operator(direction)
        alpha = norm_now / lax.optimization_barrier(jnp.sum(direction * image, axis=1))
        solution = solution + alpha[:, None] * direction
        residual = residual - alpha[:, None] * image
        if step + 1 < ITERS:
            norm_next = lax.optimization_barrier(jnp.sum(residual * residual, axis=1))
            direction = residual + (norm_next / norm_now)[:, None] * direction
            norm_now = norm_next
    return (solution, residual)
```

```python
import functools
import math

import jax
import jax.numpy as jnp
from jax import lax
from jax.experimental import pallas as pl
from jax.experimental.pallas import tpu as pltpu
from jax.sharding import PartitionSpec as P

ITERS = 3
F32 = jnp.float32
BF16 = jnp.bfloat16
MESH = pl.DeviceIdType.MESH
LN2 = math.log(2.0)
SPREAD = math.sqrt(5.0) / LN2
LINEAR = 3.0 / LN2
CONSTANT = 3.0 / LN2**2
CHUNK = 512


def pieces(x):
    first = x.astype(BF16).astype(F32)
    rest = x - first
    second = rest.astype(BF16).astype(F32)
    return first, second, (rest - second).astype(BF16).astype(F32)


def with_norms(x, before, after):
    parts = pieces(jnp.sum(x * x, axis=0, keepdims=True))
    row = lax.broadcasted_iota(jnp.int32, x.shape, 0)
    out = jnp.where((row >= after) & (row < after + 3), 1.0, 0.0)
    for i, part in enumerate(parts):
        out = jnp.where(row == before + i, part, out)
    return out


def left_operand(x):
    one, two, three = (-2.0 * p for p in pieces(x))
    return jnp.concatenate([one, one, two, two, one, three, with_norms(x, 0, 3), jnp.zeros_like(x)], axis=0)


def right_operand(x):
    one, two, three = pieces(x)
    return jnp.concatenate([one, two, one, two, three, one, with_norms(x, 3, 0), jnp.zeros_like(x)], axis=0)


def dot(a, b):
    return lax.dot_general(a, b, (((1,), (0,)), ((), ())), preferred_element_type=F32)


def kernel(rows, cols, points, scales, signal, noise, targets, bits, out_x, out_r,
           mine, near, far, left, right, upper, lower, even, odd, vectors, resid, direc, steps, part, landed, images, tell, told,
           near_sem, far_sem, land_sem, image_sem, told_sem, sent):
    n = points.shape[1]
    pairs = rows // 2
    width = 2 * n
    depth = cols * n
    chunks = depth // CHUNK
    row, col = lax.axis_index("row"), lax.axis_index("col")
    here = row * cols + col
    count = rows * cols

    def remote(src, dst, send, recv, r, c):
        return pltpu.make_async_remote_copy(
            src_ref=src, dst_ref=dst, send_sem=send, recv_sem=recv, device_id={"row": r, "col": c}, device_id_type=MESH)

    def await_bytes(ref, sem):
        pltpu.make_async_copy(ref, ref, sem).wait()

    def each(lo, hi, fn):
        def step(i, carry):
            fn(i)
            return carry
        lax.fori_loop(lo, hi, step, 0)

    barrier = pltpu.get_barrier_semaphore()

    def greet(i):
        t = lax.rem(here + i, count)
        pl.semaphore_signal(barrier, inc=1, device_id={"row": t // cols, "col": lax.rem(t, cols)}, device_id_type=MESH)

    each(1, count, greet)
    mine[0:16, :] = points[...] / scales[...] * SPREAD
    mine[16:17, :] = targets[...]
    mine[17:48, :] = 2.0 * bits[...].astype(F32) - 1.0
    near[col] = mine[...]
    far[row] = mine[0:16, :]
    steps[...] = jnp.zeros_like(steps)
    pl.semaphore_wait(barrier, count - 1)

    def send_near(i):
        c = lax.rem(col + i, cols)
        remote(mine, near.at[col], sent.at[0], near_sem.at[col], row, c).start()

    def send_far(i):
        r = lax.rem(row + i, rows)
        remote(mine.at[0:16], far.at[row], sent.at[1], far_sem.at[row], r, col).start()

    each(1, rows, send_far)
    each(1, cols, send_near)

    def split_into(j, d):
        at = pl.ds(pl.multiple_of(j * n, n), n)
        one, two, three = pieces(d)
        vectors[0:32, at] = one.astype(BF16)
        vectors[32:64, at] = two.astype(BF16)
        vectors[64:96, at] = three.astype(BF16)

    def take_near(i):
        j = lax.rem(col + i, cols)

        @pl.when(i > 0)
        def _():
            remote(mine, near.at[j], sent.at[0], near_sem.at[j], row, j).wait_recv()

        block = near[j]
        left[pl.ds(pl.multiple_of(j * n, n), n), :] = jnp.transpose(left_operand(block[0:16])).astype(BF16)
        resid[j] = block[16:48]
        direc[j] = block[16:48]
        split_into(j, block[16:48])

    def take_far(i):
        j = lax.rem(row + i, rows)

        @pl.when(i > 0)
        def _():
            remote(mine.at[0:16], far.at[j], sent.at[1], far_sem.at[j], j, col).wait_recv()

        right[j // 2, :, pl.ds(pl.multiple_of(lax.rem(j, 2) * n, n), n)] = right_operand(far[j]).astype(BF16)

    each(0, rows, take_far)
    each(0, cols, take_near)

    amplitude = jnp.log(jnp.full((1, width), signal[0], F32)) * (1.0 / LN2) - math.log2(CONSTANT)

    def distances(p, c):
        return dot(left[pl.ds(pl.multiple_of(c * CHUNK, CHUNK), CHUNK), :], right[p])

    def evaluate(buffer, p, c):
        for at in range(0, CHUNK, 32):
            u = jnp.maximum(buffer[at : at + 32, :], 1e-30)
            q = u * lax.rsqrt(u)
            value = ((q + LINEAR) * q + CONSTANT) * jnp.exp2(amplitude - q)
            high = value.astype(BF16)
            to = pl.ds(pl.multiple_of(c * CHUNK + at, 32), 32)
            upper[p, to, :] = high
            lower[p, to, :] = (value - high.astype(F32)).astype(BF16)

    def build(p):
        even[...] = distances(p, 0)

        def step(i):
            odd[...] = distances(p, 2 * i + 1)
            evaluate(even, p, 2 * i)
            even[...] = distances(p, lax.rem(2 * i + 2, chunks))
            evaluate(odd, p, 2 * i + 1)

        each(0, chunks // 2, step)

    each(0, pairs, build)

    def image_at_home(k):
        def step(s):
            p = lax.rem(row // 2 + 1 + s, pairs)
            big = dot(vectors[...], upper[p])
            small = dot(vectors[0:64, :], lower[p])
            total = big[0:32] + (big[32:64] + small[0:32] + (big[64:96] + small[32:64]))
            for core in range(2):
                r = 2 * p + core
                part[k, r] = total[:, core * n : core * n + n]

                @pl.when(r != row)
                def _():
                    slot = lax.rem(row - r + 2 * rows - 1, rows)
                    remote(part.at[k, r], landed.at[k, slot], sent.at[2 + k], land_sem.at[k], r, col).start()

        each(0, pairs, step)
        await_bytes(landed.at[k], land_sem.at[k])
        total = part[k, row]
        for slot in range(rows - 1):
            total = total + landed[k, slot]
        return total + noise[0] * direc[col]

    for k in range(ITERS):
        image = image_at_home(k)
        d, r = direc[col], resid[col]
        sums = [jnp.sum(a, axis=1, keepdims=True) for a in (d * image, r * image, image * image, r * r)]
        turned = jnp.transpose(jnp.broadcast_to(jnp.concatenate(sums, axis=0), (128, 128)))
        tell[k, 0:1] = turned[0:1]
        told[k, pl.ds(here, 1)] = turned[0:1]

        def send_tell(i):
            t = lax.rem(here + i, count)
            remote(tell.at[k, 0:1], told.at[k, pl.ds(here, 1)], sent.at[5 + k], told_sem.at[k],
                   t // cols, lax.rem(t, cols)).start()

        each(1, count, send_tell)
        if k + 1 < ITERS:
            images[k, col] = image

            def send_image(i):
                c = lax.rem(col + i, cols)
                remote(images.at[k, col], images.at[k, col], sent.at[8 + k], image_sem.at[k, col], row, c).start()

            each(1, cols, send_image)
        await_bytes(told.at[k, 0 : count - 1], told_sem.at[k])
        total = jnp.sum(told[k], axis=0, keepdims=True)
        turned = jnp.transpose(jnp.broadcast_to(total, (128, 128)))
        curved, mixed, square, norm = (turned[32 * i : 32 * i + 32] for i in range(4))
        alpha = norm / curved
        following = norm - 2.0 * alpha * mixed + alpha * alpha * square
        beta = following / norm
        alpha = jnp.concatenate([alpha] * (n // 128), axis=1)
        beta = jnp.concatenate([beta] * (n // 128), axis=1)
        steps[...] = steps[...] + alpha * d
        if k + 1 == ITERS:
            out_x[...] = steps[...]
            out_r[...] = r - alpha * image
        else:
            def take_image(i):
                j = lax.rem(col + i, cols)

                @pl.when(i > 0)
                def _():
                    remote(images.at[k, j], images.at[k, j], sent.at[8 + k], image_sem.at[k, j], row, j).wait_recv()

                rest = resid[j] - alpha * images[k, j]
                onward = rest + beta * direc[j]
                resid[j] = rest
                direc[j] = onward
                split_into(j, onward)

            each(0, cols, take_image)

    await_bytes(near.at[0 : cols - 1], sent.at[0])
    await_bytes(far.at[0 : rows - 1], sent.at[1])
    for k in range(ITERS):
        await_bytes(landed.at[k], sent.at[2 + k])
        await_bytes(told.at[k, 0 : count - 1], sent.at[5 + k])
        if k + 1 < ITERS:
            await_bytes(images.at[k, 0 : cols - 1], sent.at[8 + k])


def solution(mesh):
    rows, cols = mesh.shape["row"], mesh.shape["col"]
    pairs = rows // 2

    def body(points, lengthscale, signal, noise, targets, probe_bits):
        n = points.shape[1]
        depth, width, block = cols * n, 2 * n, (32, n)
        vmem = pl.BlockSpec(memory_space=pltpu.VMEM)
        smem = pl.BlockSpec(memory_space=pltpu.SMEM)
        return pl.pallas_call(
            functools.partial(kernel, rows, cols),
            out_shape=(jax.ShapeDtypeStruct(block, F32),) * 2,
            in_specs=[vmem, vmem, smem, smem, vmem, vmem],
            out_specs=(vmem, vmem),
            scratch_shapes=[
                pltpu.VMEM((48, n), F32),
                pltpu.VMEM((cols, 48, n), F32),
                pltpu.VMEM((rows, 16, n), F32),
                pltpu.VMEM((depth, 128), BF16),
                pltpu.VMEM((pairs, 128, width), BF16),
                pltpu.VMEM((pairs, depth, width), BF16),
                pltpu.VMEM((pairs, depth, width), BF16),
                pltpu.VMEM((CHUNK, width), F32),
                pltpu.VMEM((CHUNK, width), F32),
                pltpu.VMEM((96, depth), BF16),
                pltpu.VMEM((cols, *block), F32),
                pltpu.VMEM((cols, *block), F32),
                pltpu.VMEM(block, F32),
                pltpu.VMEM((ITERS, rows, *block), F32),
                pltpu.VMEM((ITERS, rows - 1, *block), F32),
                pltpu.VMEM((ITERS - 1, cols, *block), F32),
                pltpu.VMEM((ITERS, 8, 128), F32),
                pltpu.VMEM((ITERS, rows * cols, 128), F32),
                pltpu.SemaphoreType.DMA((cols,)),
                pltpu.SemaphoreType.DMA((rows,)),
                pltpu.SemaphoreType.DMA((ITERS,)),
                pltpu.SemaphoreType.DMA((ITERS - 1, cols)),
                pltpu.SemaphoreType.DMA((ITERS,)),
                pltpu.SemaphoreType.DMA((10,)),
            ],
            compiler_params=pltpu.CompilerParams(
                collective_id=0, has_side_effects=True, vmem_limit_bytes=60 * 1024 * 1024),
        )(points, lengthscale[:, None], signal, noise, targets[None, :], probe_bits)

    both = ("row", "col")
    placed = (P(None, both), P(), P(), P(), P(both), P(None, both))
    return jax.shard_map(body, mesh=mesh, in_specs=placed, out_specs=(P(None, both),) * 2, check_vma=False)
```

```python
import functools
import math

import jax
import jax.numpy as jnp
from jax import lax
from jax.experimental import pallas as pl
from jax.experimental.pallas import tpu as pltpu
from jax.sharding import PartitionSpec as P

F32 = jnp.float32
BF16 = jnp.bfloat16
MESH = pl.DeviceIdType.MESH
LN2 = math.log(2.0)
SPREAD = math.sqrt(5.0) / LN2
LINEAR = 3.0 / LN2
CONSTANT = 3.0 / LN2**2
CHUNK = 512


def pieces(x):
    first = x.astype(BF16).astype(F32)
    rest = x - first
    second = rest.astype(BF16).astype(F32)
    return first, second, (rest - second).astype(BF16).astype(F32)


def with_norms(x, before, after):
    parts = pieces(jnp.sum(x * x, axis=0, keepdims=True))
    row = lax.broadcasted_iota(jnp.int32, x.shape, 0)
    out = jnp.where((row >= after) & (row < after + 3), 1.0, 0.0)
    for i, part in enumerate(parts):
        out = jnp.where(row == before + i, part, out)
    return out


def left_operand(x):
    one, two, three = (-2.0 * p for p in pieces(x))
    return jnp.concatenate([one, one, two, two, one, three, with_norms(x, 0, 3), jnp.zeros_like(x)], axis=0)


def right_operand(x):
    one, two, three = pieces(x)
    return jnp.concatenate([one, two, one, two, three, one, with_norms(x, 3, 0), jnp.zeros_like(x)], axis=0)


def dot(a, b):
    return lax.dot_general(a, b, (((1,), (0,)), ((), ())), preferred_element_type=F32)


def flipped(v):
    return v + 1 - 2 * lax.rem(v, 2)


def turned(v):
    return lax.rem(v + 2 * lax.rem(v, 2) + 3, 4)


def kernel(rings, points, scales, signal, noise, targets, bits, out_x, out_r,
           mine, mine_b, near, near_b, far, left, right, upper, lower, even, odd, vectors, sums, part, landed, gathered,
           met, summed, near_sem, far_sem, land_sem, gather_sem, relay_sem, met_sem, summed_sem, sent):
    n = points.shape[1]
    cube = 2**rings
    pairs = cube // 2
    width = 2 * n
    depth = 2 * cube * n
    chunks = depth // CHUNK
    row, col = lax.axis_index("row"), lax.axis_index("col")
    core = lax.rem(row, 2)
    place = [row // 2]
    for i in range(rings - 1):
        place.append(lax.rem(col // 4 ** (rings - 2 - i), 4))

    def device(places, core):
        c = 0
        for v in places[1:]:
            c = 4 * c + v
        return {"row": 2 * places[0] + core, "col": c}

    def gather_partner(mask, other):
        return device([flipped(v) if mask >> i & 1 else v for i, v in enumerate(place)], 1 - core if other else core)

    def reduce_partner(mask):
        return device([v + lax.rem(mask // 2**i, 2) * (turned(v) - v) for i, v in enumerate(place)], core)

    def remote(src, dst, send, recv, to):
        return pltpu.make_async_remote_copy(
            src_ref=src, dst_ref=dst, send_sem=send, recv_sem=recv, device_id=to, device_id_type=MESH)

    def await_bytes(ref, sem):
        pltpu.make_async_copy(ref, ref, sem).wait()

    def each(lo, hi, fn):
        def step(i, carry):
            fn(i)
            return carry
        lax.fori_loop(lo, hi, step, 0)

    near_masks = sorted(range(1, cube), key=lambda m: (-bin(m).count("1"), m))
    slots = [(m, f) for m in near_masks for f in range(2)] + [(0, 1)]

    barrier = pltpu.get_barrier_semaphore()
    for m, f in slots:
        pl.semaphore_signal(barrier, inc=1, device_id=gather_partner(m, f), device_id_type=MESH)
    for m in near_masks:
        pl.semaphore_signal(barrier, inc=1, device_id=reduce_partner(m), device_id_type=MESH)
    x = points[...] / scales[...] * SPREAD
    mine[...] = x
    near[0] = x
    far[cube - 1] = x
    mine_b[0:1, :] = targets[...]
    mine_b[1:32, :] = 2.0 * bits[...].astype(F32) - 1.0
    near_b[0] = mine_b[...]
    pl.semaphore_wait(barrier, len(slots) + len(near_masks))

    for m, f in slots:
        remote(mine, near.at[f * cube + m], sent.at[0], near_sem.at[0], gather_partner(m, f)).start()
    for m in near_masks:
        remote(mine, far.at[cube - 1 - m], sent.at[1], far_sem.at[0], reduce_partner(m)).start()
    for m, f in slots:
        remote(mine_b, near_b.at[f * cube + m], sent.at[2], near_sem.at[1], gather_partner(m, f)).start()

    def split_into(slot, d):
        at = pl.ds(pl.multiple_of(slot * n, n), n)
        high = d.astype(BF16)
        vectors[0:32, at] = high
        vectors[32:64, at] = (d - high.astype(F32)).astype(BF16)

    def place_left(i):
        left[pl.ds(pl.multiple_of(i * n, n), n), :] = jnp.transpose(left_operand(near[i])).astype(BF16)

    def place_right(i):
        right[i // 2, :, pl.ds(pl.multiple_of(lax.rem(i, 2) * n, n), n)] = right_operand(far[i]).astype(BF16)

    await_bytes(far.at[0 : cube - 1], far_sem.at[0])
    each(0, cube, place_right)
    await_bytes(near.at[1 : 2 * cube], near_sem.at[0])
    each(0, 2 * cube, place_left)

    amplitude = jnp.log(jnp.full((1, width), signal[0], F32)) * (1.0 / LN2) - math.log2(CONSTANT)

    def distances(p, c):
        return dot(left[pl.ds(pl.multiple_of(c * CHUNK, CHUNK), CHUNK), :], right[p])

    def evaluate(buffer, p, c):
        for at in range(0, CHUNK, 32):
            u = jnp.maximum(buffer[at : at + 32, :], 1e-30)
            q = u * lax.rsqrt(u)
            value = ((q + LINEAR) * q + CONSTANT) * jnp.exp2(amplitude - q)
            high = value.astype(BF16)
            to = pl.ds(pl.multiple_of(c * CHUNK + at, 32), 32)
            upper[p, to, :] = high
            lower[p, to, :] = (value - high.astype(F32)).astype(BF16)

    def product(p, at):
        big = dot(vectors[:, at], upper[p, at, :])
        small = dot(vectors[0:32, at], lower[p, at, :])
        return big[0:32] + (big[32:64] + small)

    def send_parts(k, p, total):
        for j in range(2):
            slot = 2 * p + j
            part[k, slot] = total[:, j * n : j * n + n]

            def send():
                remote(part.at[k, slot], landed.at[k, slot], sent.at[3 + k], land_sem.at[k],
                       reduce_partner(cube - 1 - slot)).start()

            if isinstance(p, int):
                if slot < cube - 1:
                    send()
            elif j == 0:
                send()
            else:
                pl.when(p < pairs - 1)(send)

    even[...] = distances(0, 0)
    for p in range(pairs):
        if p == 1:
            await_bytes(near_b.at[1 : 2 * cube], near_sem.at[1])
            each(0, 2 * cube, lambda i: split_into(i, near_b[i]))
        if p:
            sums[...] = jnp.zeros_like(sums)

        def step(i):
            odd[...] = distances(p, 2 * i + 1)
            evaluate(even, p, 2 * i)
            even[...] = distances(jnp.minimum(p + (2 * i + 2) // chunks, pairs - 1), lax.rem(2 * i + 2, chunks))
            evaluate(odd, p, 2 * i + 1)
            if p:
                sums[...] = sums[...] + product(p - 1, pl.ds(pl.multiple_of(2 * i * CHUNK, 2 * CHUNK), 2 * CHUNK))

        each(0, chunks // 2, step)
        if p:
            send_parts(0, p - 1, sums[...])
    if pairs == 1:
        await_bytes(near_b.at[1 : 2 * cube], near_sem.at[1])
        each(0, 2 * cube, lambda i: split_into(i, near_b[i]))
    send_parts(0, pairs - 1, product(pairs - 1, pl.ds(0, depth)))

    def multiply(k):
        each(0, pairs, lambda p: send_parts(k, p, product(p, pl.ds(0, depth))))

    def at_home(k, v):
        await_bytes(landed.at[k], land_sem.at[k])
        total = part[k, cube - 1]
        for slot in range(cube - 1):
            total = total + landed[k, slot]
        return total + noise[0] * v

    def gather(k, w):
        gathered[k, 0] = w
        for m in near_masks:
            remote(gathered.at[k, 0], gathered.at[k, m], sent.at[6 + k], gather_sem.at[k, m], gather_partner(m, 0)).start()
        remote(gathered.at[k, 0], gathered.at[k, cube], sent.at[6 + k], relay_sem.at[k], gather_partner(0, 1)).start()

    def take_gathered(k):
        split_into(0, gathered[k, 0])
        for m in reversed(near_masks):
            remote(gathered.at[k, 0], gathered.at[k, m], sent.at[6 + k], gather_sem.at[k, m], gather_partner(m, 0)).wait_recv()
            remote(gathered.at[k, m], gathered.at[k, cube + m], sent.at[6 + k], relay_sem.at[k], gather_partner(0, 1)).start()
            split_into(m, gathered[k, m])
        await_bytes(gathered.at[k, cube : 2 * cube], relay_sem.at[k])
        each(cube, 2 * cube, lambda i: split_into(i, gathered[k, i]))

    def tell(k, r, w):
        both = [jnp.sum(a, axis=1, keepdims=True) for a in (r * r, w * r)]
        column = jnp.concatenate(both + [jnp.zeros((64, 1), F32)], axis=0)
        met[k, 0:1] = jnp.transpose(jnp.broadcast_to(column, (128, 128)))[0:1]
        for m, f in slots:
            at = f * cube + m
            remote(met.at[k, 0:1], met.at[k, at : at + 1], sent.at[8 + k], met_sem.at[k], gather_partner(m, f)).start()

    def pass_on(k):
        await_bytes(met.at[k, 1 : 2 * cube], met_sem.at[k])
        summed[k, cube - 1 : cube] = jnp.sum(met[k], axis=0, keepdims=True)
        for m in near_masks:
            at = cube - 1 - m
            remote(summed.at[k, cube - 1 : cube], summed.at[k, at : at + 1], sent.at[11 + k], summed_sem.at[k],
                   reduce_partner(m)).start()

    def hear(k):
        await_bytes(summed.at[k, 0 : cube - 1], summed_sem.at[k])
        total = jnp.sum(summed[k], axis=0, keepdims=True)
        spread = jnp.transpose(jnp.broadcast_to(total, (128, 128)))
        return [jnp.concatenate([spread[32 * i : 32 * i + 32]] * (n // 128), axis=1) for i in range(2)]

    r = near_b[0]
    w = at_home(0, r)
    gather(0, w)
    tell(0, r, w)
    take_gathered(0)
    pass_on(0)
    multiply(1)
    z = at_home(1, w)
    norm, curved = hear(0)
    alpha = norm / curved
    p, s = r, w
    r, w_next = r - alpha * s, w - alpha * z
    gather(1, w_next)
    tell(1, r, w_next)
    x = alpha * p
    take_gathered(1)
    pass_on(1)
    multiply(2)
    w = w_next
    q = at_home(2, w)
    following, curved = hear(1)
    beta = following / norm
    norm, alpha = following, following / (curved - beta * following / alpha)
    p, s, z = r + beta * p, w + beta * s, q + beta * z
    r, w = r - alpha * s, w - alpha * z
    tell(2, r, w)
    x = x + alpha * p
    pass_on(2)
    following, curved = hear(2)
    beta = following / norm
    alpha = following / (curved - beta * following / alpha)
    out_x[...] = x + alpha * (r + beta * p)
    out_r[...] = r - alpha * (w + beta * s)

    await_bytes(near.at[1 : 2 * cube], sent.at[0])
    await_bytes(far.at[0 : cube - 1], sent.at[1])
    await_bytes(near_b.at[1 : 2 * cube], sent.at[2])
    for k in range(3):
        await_bytes(landed.at[k], sent.at[3 + k])
        await_bytes(met.at[k, 1 : 2 * cube], sent.at[8 + k])
        await_bytes(summed.at[k, 0 : cube - 1], sent.at[11 + k])
    for k in range(2):
        await_bytes(gathered.at[k, 1 : 2 * cube], sent.at[6 + k])


def solution(mesh):
    rings = {1: 1, 4: 2, 16: 3}[mesh.shape["col"]]
    cube = 2**rings

    def body(points, lengthscale, signal, noise, targets, probe_bits):
        n = points.shape[1]
        depth, width, block = 2 * cube * n, 2 * n, (32, n)
        vmem = pl.BlockSpec(memory_space=pltpu.VMEM)
        smem = pl.BlockSpec(memory_space=pltpu.SMEM)
        return pl.pallas_call(
            functools.partial(kernel, rings),
            out_shape=(jax.ShapeDtypeStruct(block, F32),) * 2,
            in_specs=[vmem, vmem, smem, smem, vmem, vmem],
            out_specs=(vmem, vmem),
            scratch_shapes=[
                pltpu.VMEM((16, n), F32),
                pltpu.VMEM(block, F32),
                pltpu.VMEM((2 * cube, 16, n), F32),
                pltpu.VMEM((2 * cube, *block), F32),
                pltpu.VMEM((cube, 16, n), F32),
                pltpu.VMEM((depth, 128), BF16),
                pltpu.VMEM((cube // 2, 128, width), BF16),
                pltpu.VMEM((cube // 2, depth, width), BF16),
                pltpu.VMEM((cube // 2, depth, width), BF16),
                pltpu.VMEM((CHUNK, width), F32),
                pltpu.VMEM((CHUNK, width), F32),
                pltpu.VMEM((64, depth), BF16),
                pltpu.VMEM((32, width), F32),
                pltpu.VMEM((3, cube, *block), F32),
                pltpu.VMEM((3, cube - 1, *block), F32),
                pltpu.VMEM((2, 2 * cube, *block), F32),
                pltpu.VMEM((3, 2 * cube, 128), F32),
                pltpu.VMEM((3, cube, 128), F32),
                pltpu.SemaphoreType.DMA((2,)),
                pltpu.SemaphoreType.DMA((1,)),
                pltpu.SemaphoreType.DMA((3,)),
                pltpu.SemaphoreType.DMA((2, cube)),
                pltpu.SemaphoreType.DMA((2,)),
                pltpu.SemaphoreType.DMA((3,)),
                pltpu.SemaphoreType.DMA((3,)),
                pltpu.SemaphoreType.DMA((14,)),
            ],
            compiler_params=pltpu.CompilerParams(
                collective_id=0, has_side_effects=True, vmem_limit_bytes=60 * 1024 * 1024),
        )(points, lengthscale[:, None], signal, noise, targets[None, :], probe_bits)

    both = ("row", "col")
    placed = (P(None, both), P(), P(), P(), P(both), P(None, both))
    return jax.shard_map(body, mesh=mesh, in_specs=placed, out_specs=(P(None, both),) * 2, check_vma=False)
```

```python
import functools
import math

import jax
import jax.numpy as jnp
from jax import lax
from jax.experimental import pallas as pl
from jax.experimental.pallas import tpu as pltpu
from jax.sharding import PartitionSpec as P

F32 = jnp.float32
BF16 = jnp.bfloat16
MESH = pl.DeviceIdType.MESH
LN2 = math.log(2.0)
SPREAD = math.sqrt(5.0) / LN2
LINEAR = 3.0 / LN2
CONSTANT = 3.0 / LN2**2
CHUNK = 512


def pieces(x):
    first = x.astype(BF16).astype(F32)
    rest = x - first
    second = rest.astype(BF16).astype(F32)
    return first, second, (rest - second).astype(BF16).astype(F32)


def with_norms(x, before, after):
    parts = pieces(jnp.sum(x * x, axis=0, keepdims=True))
    row = lax.broadcasted_iota(jnp.int32, x.shape, 0)
    out = jnp.where((row >= after) & (row < after + 3), 1.0, 0.0)
    for i, part in enumerate(parts):
        out = jnp.where(row == before + i, part, out)
    return out


def left_operand(x):
    one, two, three = (-2.0 * p for p in pieces(x))
    return jnp.concatenate([one, one, two, two, one, three, with_norms(x, 0, 3), jnp.zeros_like(x)], axis=0)


def right_operand(x):
    one, two, three = pieces(x)
    return jnp.concatenate([one, two, one, two, three, one, with_norms(x, 3, 0), jnp.zeros_like(x)], axis=0)


def dot(a, b):
    return lax.dot_general(a, b, (((1,), (0,)), ((), ())), preferred_element_type=F32)


def flipped(v):
    return v + 1 - 2 * lax.rem(v, 2)


def turned(v):
    return lax.rem(v + 2 * lax.rem(v, 2) + 3, 4)


def kernel(rings, points, scales, signal, noise, targets, bits, out_x, out_r, out_dx, out_dr,
           points_here, scales_here, targets_here, bits_here, fetched, mine, mine_b, near, near_b, far, left, right, upper, lower, even, odd, vectors, sums, part, landed, gathered,
           met, summed, halves, near_b_sem, near_sem, far_sem, land_sem, gather_sem, relay_sem, met_sem, summed_sem, sent):
    n = points_here.shape[1]
    cube = 2**rings
    pairs = cube // 2
    width = 2 * n
    depth = 2 * cube * n
    chunks = depth // CHUNK
    row, col = lax.axis_index("row"), lax.axis_index("col")
    core = lax.rem(row, 2)
    place = [row // 2]
    for i in range(rings - 1):
        place.append(lax.rem(col // 4 ** (rings - 2 - i), 4))

    def device(places, core):
        c = 0
        for v in places[1:]:
            c = 4 * c + v
        return {"row": 2 * places[0] + core, "col": c}

    def gather_partner(mask, other):
        return device([flipped(v) if mask >> i & 1 else v for i, v in enumerate(place)], 1 - core if other else core)

    def reduce_partner(mask):
        return device([v + lax.rem(mask // 2**i, 2) * (turned(v) - v) for i, v in enumerate(place)], core)

    def remote(src, dst, send, recv, to):
        return pltpu.make_async_remote_copy(
            src_ref=src, dst_ref=dst, send_sem=send, recv_sem=recv, device_id=to, device_id_type=MESH)

    def await_bytes(ref, sem):
        pltpu.make_async_copy(ref, ref, sem).wait()

    def each(lo, hi, fn):
        def step(i, carry):
            fn(i)
            return carry
        lax.fori_loop(lo, hi, step, 0)

    near_masks = sorted(range(1, cube), key=lambda m: (-bin(m).count("1"), m))
    slots = [(m, f) for m in near_masks for f in range(2)] + [(0, 1)]

    barrier = pltpu.get_barrier_semaphore()
    for m, f in slots:
        pl.semaphore_signal(barrier, inc=1, device_id=gather_partner(m, f), device_id_type=MESH)
    for m in near_masks:
        pl.semaphore_signal(barrier, inc=1, device_id=reduce_partner(m), device_id_type=MESH)
    local = [pltpu.make_async_copy(src, dst, fetched.at[i])
             for i, (src, dst) in enumerate(((points, points_here), (scales, scales_here), (targets, targets_here), (bits, bits_here)))]
    for copy in local:
        copy.start()
    for copy in local:
        copy.wait()
    diagonal = lax.broadcasted_iota(jnp.int32, (16, 16), 0) == lax.broadcasted_iota(jnp.int32, (16, 16), 1)
    scale = jnp.sum(jnp.where(diagonal, scales_here[...], 0.0), axis=1, keepdims=True)
    x = points_here[...] / scale * SPREAD
    mine[...] = x
    near[0] = x
    far[cube - 1] = x
    mine_b[0:1, :] = targets_here[...]
    mine_b[1:32, :] = 2.0 * bits_here[...].astype(F32) - 1.0
    near_b[0] = mine_b[...]
    pl.semaphore_wait(barrier, len(slots) + len(near_masks))

    def send_near(m, f):
        return remote(mine, near.at[f * cube + m], sent.at[0], near_sem.at[f * cube + m], gather_partner(m, f))

    for m in near_masks:
        remote(mine, far.at[cube - 1 - m], sent.at[1], far_sem.at[0], reduce_partner(m)).start()
    for m, f in slots:
        send_near(m, f).start()
    for m, f in slots:
        remote(mine_b, near_b.at[f * cube + m], sent.at[2], near_b_sem.at[0], gather_partner(m, f)).start()

    def split_into(slot, d):
        at = pl.ds(pl.multiple_of(slot * n, n), n)
        high = d.astype(BF16)
        vectors[0:32, at] = high
        vectors[32:64, at] = (d - high.astype(F32)).astype(BF16)

    def place_left(i):
        left[i * n : i * n + n, :] = jnp.transpose(left_operand(near[i])).astype(BF16)

    def place_right(i):
        right[i // 2, :, pl.ds(pl.multiple_of(lax.rem(i, 2) * n, n), n)] = right_operand(far[i]).astype(BF16)

    place_left(0)
    for m, f in reversed(slots):
        send_near(m, f).wait_recv()
        place_left(f * cube + m)
    await_bytes(far.at[0 : cube - 1], far_sem.at[0])
    each(0, cube, place_right)

    def distances(p, c):
        return dot(left[pl.ds(pl.multiple_of(c * CHUNK, CHUNK), CHUNK), :], right[p])

    def evaluate(buffer, p, c):
        for at in range(0, CHUNK, 32):
            u = jnp.maximum(buffer[at : at + 32, :], 1e-30)
            q = u * lax.rsqrt(u)
            value = ((q + LINEAR) * q + CONSTANT) * jnp.exp2(-math.log2(CONSTANT) - q)
            high = value.astype(BF16)
            to = pl.ds(pl.multiple_of(c * CHUNK + at, 32), 32)
            upper[p, to, :] = high
            lower[p, to, :] = (value - upper[p, to, :].astype(F32)).astype(BF16)

    def product(p, at):
        big = dot(vectors[:, at], upper[p, at, :])
        small = dot(vectors[0:32, at], lower[p, at, :])
        return big[0:32] + (big[32:64] + small)

    def send_parts(k, p, total):
        for j in range(2):
            slot = 2 * p + j
            part[k, slot] = total[:, j * n : j * n + n]

            def send():
                remote(part.at[k, slot], landed.at[k, slot], sent.at[3 + k], land_sem.at[k],
                       reduce_partner(cube - 1 - slot)).start()

            if isinstance(p, int):
                if slot < cube - 1:
                    send()
            elif j == 0:
                send()
            else:
                pl.when(p < pairs - 1)(send)

    even[...] = distances(0, 0)
    for p in range(pairs):
        if p == 1:
            await_bytes(near_b.at[1 : 2 * cube], near_b_sem.at[0])
            each(0, 2 * cube, lambda i: split_into(i, near_b[i]))
        if p:
            sums[...] = jnp.zeros_like(sums)

        def step(i):
            odd[...] = distances(p, 2 * i + 1)
            evaluate(even, p, 2 * i)
            even[...] = distances(jnp.minimum(p + (2 * i + 2) // chunks, pairs - 1), lax.rem(2 * i + 2, chunks))
            evaluate(odd, p, 2 * i + 1)
            if p:
                sums[...] = sums[...] + product(p - 1, pl.ds(pl.multiple_of(2 * i * CHUNK, 2 * CHUNK), 2 * CHUNK))

        each(0, chunks // 2, step)
        if p:
            send_parts(0, p - 1, sums[...])
    if pairs == 1:
        await_bytes(near_b.at[1 : 2 * cube], near_b_sem.at[0])
        each(0, 2 * cube, lambda i: split_into(i, near_b[i]))
    send_parts(0, pairs - 1, product(pairs - 1, pl.ds(0, depth)))

    def multiply(k):
        half = depth // 2

        def first(p):
            halves[p] = product(p, pl.ds(0, half))

        each(0, pairs, first)
        take_relayed(k - 1)
        pass_on(k - 1)
        each(0, pairs, lambda p: send_parts(k, p, halves[p] + product(p, pl.ds(half, half))))

    def at_home(k, v):
        await_bytes(landed.at[k], land_sem.at[k])
        total = part[k, cube - 1]
        for slot in range(cube - 1):
            total = total + landed[k, slot]
        return signal[0] * total + noise[0] * v

    def gather(k, w):
        gathered[k, 0] = w
        for m in near_masks:
            remote(gathered.at[k, 0], gathered.at[k, m], sent.at[6 + k], gather_sem.at[k, m], gather_partner(m, 0)).start()
        remote(gathered.at[k, 0], gathered.at[k, cube], sent.at[6 + k], relay_sem.at[k], gather_partner(0, 1)).start()

    def take_gathered(k):
        split_into(0, gathered[k, 0])
        for m in reversed(near_masks):
            remote(gathered.at[k, 0], gathered.at[k, m], sent.at[6 + k], gather_sem.at[k, m], gather_partner(m, 0)).wait_recv()
            remote(gathered.at[k, m], gathered.at[k, cube + m], sent.at[6 + k], relay_sem.at[k], gather_partner(0, 1)).start()
            split_into(m, gathered[k, m])

    def take_relayed(k):
        await_bytes(gathered.at[k, cube : 2 * cube], relay_sem.at[k])
        each(cube, 2 * cube, lambda i: split_into(i, gathered[k, i]))

    def tell(k, r, w):
        both = [jnp.sum(a, axis=1, keepdims=True) for a in (r * r, w * r)]
        column = jnp.concatenate(both + [jnp.zeros((64, 1), F32)], axis=0)
        met[k, 0:1] = jnp.transpose(jnp.broadcast_to(column, (128, 128)))[0:1]
        for m, f in slots:
            at = f * cube + m
            remote(met.at[k, 0:1], met.at[k, at : at + 1], sent.at[8 + k], met_sem.at[k], gather_partner(m, f)).start()

    def pass_on(k):
        await_bytes(met.at[k, 1 : 2 * cube], met_sem.at[k])
        summed[k, cube - 1 : cube] = jnp.sum(met[k], axis=0, keepdims=True)
        for m in near_masks:
            at = cube - 1 - m
            remote(summed.at[k, cube - 1 : cube], summed.at[k, at : at + 1], sent.at[11 + k], summed_sem.at[k],
                   reduce_partner(m)).start()

    def hear(k):
        await_bytes(summed.at[k, 0 : cube - 1], summed_sem.at[k])
        total = jnp.sum(summed[k], axis=0, keepdims=True)
        spread = jnp.transpose(jnp.broadcast_to(total, (128, 128)))
        return [jnp.concatenate([spread[32 * i : 32 * i + 32]] * (n // 128), axis=1) for i in range(2)]

    r = near_b[0]
    w = at_home(0, r)
    gather(0, w)
    tell(0, r, w)
    take_gathered(0)
    multiply(1)
    z = at_home(1, w)
    norm, curved = hear(0)
    alpha = norm / curved
    p, s = r, w
    r, w_next = r - alpha * s, w - alpha * z
    gather(1, w_next)
    tell(1, r, w_next)
    x = alpha * p
    take_gathered(1)
    multiply(2)
    w = w_next
    q = at_home(2, w)
    following, curved = hear(1)
    beta = following / norm
    norm, alpha = following, following / (curved - beta * following / alpha)
    p, s, z = r + beta * p, w + beta * s, q + beta * z
    r, w = r - alpha * s, w - alpha * z
    tell(2, r, w)
    x = x + alpha * p
    pass_on(2)
    following, curved = hear(2)
    beta = following / norm
    alpha = following / (curved - beta * following / alpha)
    out_x[...] = x
    out_r[...] = r
    out_dx[...] = alpha * (r + beta * p)
    out_dr[...] = alpha * (w + beta * s)

    await_bytes(near.at[1 : 2 * cube], sent.at[0])
    await_bytes(far.at[0 : cube - 1], sent.at[1])
    await_bytes(near_b.at[1 : 2 * cube], sent.at[2])
    for k in range(3):
        await_bytes(landed.at[k], sent.at[3 + k])
        await_bytes(met.at[k, 1 : 2 * cube], sent.at[8 + k])
        await_bytes(summed.at[k, 0 : cube - 1], sent.at[11 + k])
    for k in range(2):
        await_bytes(gathered.at[k, 1 : 2 * cube], sent.at[6 + k])


def solution(mesh):
    rings = {1: 1, 4: 2, 16: 3}[mesh.shape["col"]]
    cube = 2**rings

    def body(points, lengthscale, signal, noise, targets, probe_bits):
        n = points.shape[1]
        depth, width, block = 2 * cube * n, 2 * n, (32, n)
        vmem = pl.BlockSpec(memory_space=pltpu.VMEM)
        smem = pl.BlockSpec(memory_space=pltpu.SMEM)
        hbm = pl.BlockSpec(memory_space=pl.ANY)
        x, r, dx, dr = pl.pallas_call(
            functools.partial(kernel, rings),
            out_shape=(jax.ShapeDtypeStruct(block, F32),) * 4,
            in_specs=[hbm, hbm, smem, smem, hbm, hbm],
            out_specs=(vmem,) * 4,
            scratch_shapes=[
                pltpu.VMEM((16, n), F32),
                pltpu.VMEM((1, 16), F32),
                pltpu.VMEM((1, n), F32),
                pltpu.VMEM((31, n), jnp.int32),
                pltpu.SemaphoreType.DMA((4,)),
                pltpu.VMEM((16, n), F32),
                pltpu.VMEM(block, F32),
                pltpu.VMEM((2 * cube, 16, n), F32),
                pltpu.VMEM((2 * cube, *block), F32),
                pltpu.VMEM((cube, 16, n), F32),
                pltpu.VMEM((depth, 128), BF16),
                pltpu.VMEM((cube // 2, 128, width), BF16),
                pltpu.VMEM((cube // 2, depth, width), BF16),
                pltpu.VMEM((cube // 2, depth, width), BF16),
                pltpu.VMEM((CHUNK, width), F32),
                pltpu.VMEM((CHUNK, width), F32),
                pltpu.VMEM((64, depth), BF16),
                pltpu.VMEM((32, width), F32),
                pltpu.VMEM((3, cube, *block), F32),
                pltpu.VMEM((3, cube - 1, *block), F32),
                pltpu.VMEM((2, 2 * cube, *block), F32),
                pltpu.VMEM((3, 2 * cube, 128), F32),
                pltpu.VMEM((3, cube, 128), F32),
                pltpu.VMEM((cube // 2, 32, width), F32),
                pltpu.SemaphoreType.DMA((1,)),
                pltpu.SemaphoreType.DMA((2 * cube,)),
                pltpu.SemaphoreType.DMA((1,)),
                pltpu.SemaphoreType.DMA((3,)),
                pltpu.SemaphoreType.DMA((2, cube)),
                pltpu.SemaphoreType.DMA((2,)),
                pltpu.SemaphoreType.DMA((3,)),
                pltpu.SemaphoreType.DMA((3,)),
                pltpu.SemaphoreType.DMA((14,)),
            ],
            compiler_params=pltpu.CompilerParams(
                collective_id=0, has_side_effects=True,
                vmem_limit_bytes=60 * 1024 * 1024),
        )(points, lengthscale[None, :], signal, noise, targets[None, :], probe_bits)
        return x + dx, r - dr

    both = ("row", "col")
    placed = (P(None, both), P(), P(), P(), P(both), P(None, both))
    return jax.shard_map(body, mesh=mesh, in_specs=placed, out_specs=(P(None, both),) * 2, check_vma=False)
```

```python
import functools
import math

import jax
import jax.numpy as jnp
from jax import lax
from jax.experimental import pallas as pl
from jax.experimental.pallas import tpu as pltpu
from jax.sharding import PartitionSpec as P

F32 = jnp.float32
BF16 = jnp.bfloat16
MESH = pl.DeviceIdType.MESH
LN2 = math.log(2.0)
SPREAD = math.sqrt(5.0) / LN2
LINEAR = 3.0 / LN2
CONSTANT = 3.0 / LN2**2
CHUNK = 512


def pieces(x):
    first = x.astype(BF16).astype(F32)
    rest = x - first
    second = rest.astype(BF16).astype(F32)
    return first, second, (rest - second).astype(BF16).astype(F32)


def with_norms(x, before, after):
    parts = pieces(jnp.sum(x * x, axis=0, keepdims=True))
    row = lax.broadcasted_iota(jnp.int32, x.shape, 0)
    out = jnp.where((row >= after) & (row < after + 3), 1.0, 0.0)
    for i, part in enumerate(parts):
        out = jnp.where(row == before + i, part, out)
    return out


def left_operand(x):
    one, two, three = (-2.0 * p for p in pieces(x))
    return jnp.concatenate([one, one, two, two, one, three, with_norms(x, 0, 3), jnp.zeros_like(x)], axis=0)


def right_operand(x):
    one, two, three = pieces(x)
    return jnp.concatenate([one, two, one, two, three, one, with_norms(x, 3, 0), jnp.zeros_like(x)], axis=0)


def dot(a, b):
    return lax.dot_general(a, b, (((1,), (0,)), ((), ())), preferred_element_type=F32)


def flipped(v):
    return v + 1 - 2 * lax.rem(v, 2)


def turned(v):
    return lax.rem(v + 2 * lax.rem(v, 2) + 3, 4)


def kernel(rings, points, scales, signal, noise, targets, bits, out_x, out_r, out_dx, out_dr,
           points_here, scales_here, targets_here, bits_here, fetched, mine, mine_b, near, near_b, far, left, right, upper, lower, even, odd, vectors, part, landed, gathered,
           met, summed, near_b_sem, near_sem, far_sem, land_sem, gather_sem, relay_sem, met_sem, summed_sem, sent):
    n = points_here.shape[1]
    cube = 2**rings
    pairs = cube // 2
    width = 2 * n
    depth = 2 * cube * n
    chunks = depth // CHUNK
    row, col = lax.axis_index("row"), lax.axis_index("col")
    core = lax.rem(row, 2)
    place = [row // 2]
    for i in range(rings - 1):
        place.append(lax.rem(col // 4 ** (rings - 2 - i), 4))

    def device(places, core):
        c = 0
        for v in places[1:]:
            c = 4 * c + v
        return {"row": 2 * places[0] + core, "col": c}

    def gather_partner(mask, other):
        return device([flipped(v) if mask >> i & 1 else v for i, v in enumerate(place)], 1 - core if other else core)

    def reduce_partner(mask):
        return device([v + lax.rem(mask // 2**i, 2) * (turned(v) - v) for i, v in enumerate(place)], core)

    def remote(src, dst, send, recv, to):
        return pltpu.make_async_remote_copy(
            src_ref=src, dst_ref=dst, send_sem=send, recv_sem=recv, device_id=to, device_id_type=MESH)

    def await_bytes(ref, sem):
        pltpu.make_async_copy(ref, ref, sem).wait()

    def each(lo, hi, fn):
        def step(i, carry):
            fn(i)
            return carry
        lax.fori_loop(lo, hi, step, 0)

    near_masks = sorted(range(1, cube), key=lambda m: (-bin(m).count("1"), m))
    slots = [(m, f) for m in near_masks for f in range(2)] + [(0, 1)]

    barrier = pltpu.get_barrier_semaphore()
    for m, f in slots:
        pl.semaphore_signal(barrier, inc=1, device_id=gather_partner(m, f), device_id_type=MESH)
    for m in near_masks:
        pl.semaphore_signal(barrier, inc=1, device_id=reduce_partner(m), device_id_type=MESH)
    local = [pltpu.make_async_copy(src, dst, fetched.at[i])
             for i, (src, dst) in enumerate(((points, points_here), (scales, scales_here), (targets, targets_here), (bits, bits_here)))]
    for copy in local:
        copy.start()
    for copy in local:
        copy.wait()
    diagonal = lax.broadcasted_iota(jnp.int32, (16, 16), 0) == lax.broadcasted_iota(jnp.int32, (16, 16), 1)
    scale = jnp.sum(jnp.where(diagonal, scales_here[...], 0.0), axis=1, keepdims=True)
    x = points_here[...] / scale * SPREAD
    mine[...] = x
    near[0] = x
    far[cube - 1] = x
    mine_b[0:1, :] = targets_here[...]
    mine_b[1:32, :] = 2.0 * bits_here[...].astype(F32) - 1.0
    near_b[0] = mine_b[...]
    pl.semaphore_wait(barrier, len(slots) + len(near_masks))

    def send_near(m, f):
        return remote(mine, near.at[f * cube + m], sent.at[0], near_sem.at[f * cube + m], gather_partner(m, f))

    for m in near_masks:
        remote(mine, far.at[cube - 1 - m], sent.at[1], far_sem.at[0], reduce_partner(m)).start()
    for m, f in slots:
        send_near(m, f).start()
    for m, f in slots:
        remote(mine_b, near_b.at[f * cube + m], sent.at[2], near_b_sem.at[0], gather_partner(m, f)).start()

    def split_into(slot, d):
        at = pl.ds(pl.multiple_of(slot * n, n), n)
        for i, piece in enumerate(pieces(d)):
            vectors[32 * i : 32 * i + 32, at] = piece.astype(BF16)

    def place_left(i):
        left[i * n : i * n + n, :] = jnp.transpose(left_operand(near[i])).astype(BF16)

    def place_right(i):
        right[i // 2, :, pl.ds(pl.multiple_of(lax.rem(i, 2) * n, n), n)] = right_operand(far[i]).astype(BF16)

    place_left(0)
    for m, f in reversed(slots):
        send_near(m, f).wait_recv()
        place_left(f * cube + m)
    await_bytes(far.at[0 : cube - 1], far_sem.at[0])
    each(0, cube, place_right)

    def distances(p, c):
        return dot(left[pl.ds(pl.multiple_of(c * CHUNK, CHUNK), CHUNK), :], right[p])

    def evaluate(buffer, p, c):
        for at in range(0, CHUNK, 32):
            u = jnp.maximum(buffer[at : at + 32, :], 1e-30)
            q = u * lax.rsqrt(u)
            value = ((q + LINEAR) * q + CONSTANT) * jnp.exp2(-math.log2(CONSTANT) - q)
            high = value.astype(BF16)
            to = pl.ds(pl.multiple_of(c * CHUNK + at, 32), 32)
            upper[p, to, :] = high
            lower[p, to, :] = (value - upper[p, to, :].astype(F32)).astype(BF16)

    def product(p, at):
        v = vectors[:, at]
        both = dot(v, upper[p, at, :]) + dot(v, lower[p, at, :])
        return both[0:32] + (both[32:64] + both[64:96])

    def send_parts(k, p, total):
        for j in range(2):
            slot = 2 * p + j
            part[k, slot] = total[:, j * n : j * n + n]

            def send():
                remote(part.at[k, slot], landed.at[k, slot], sent.at[3 + k], land_sem.at[k],
                       reduce_partner(cube - 1 - slot)).start()

            if isinstance(p, int):
                if slot < cube - 1:
                    send()
            elif j == 0:
                send()
            else:
                pl.when(p < pairs - 1)(send)

    vectors[96:128, :] = jnp.zeros((32, depth), BF16)
    even[...] = distances(0, 0)
    def step(t):
        p, i = t // (chunks // 2), lax.rem(t, chunks // 2)
        odd[...] = distances(p, 2 * i + 1)
        evaluate(even, p, 2 * i)
        even[...] = distances(jnp.minimum(p + (2 * i + 2) // chunks, pairs - 1), lax.rem(2 * i + 2, chunks))
        evaluate(odd, p, 2 * i + 1)

    each(0, pairs * chunks // 2, step)
    await_bytes(near_b.at[1 : 2 * cube], near_b_sem.at[0])
    each(0, 2 * cube, lambda i: split_into(i, near_b[i]))
    each(0, pairs, lambda p: send_parts(0, p, product(p, pl.ds(0, depth))))

    def multiply(k):
        take_relayed(k - 1)
        pass_on(k - 1)
        each(0, pairs, lambda p: send_parts(k, p, product(p, pl.ds(0, depth))))

    def at_home(k, v):
        await_bytes(landed.at[k], land_sem.at[k])
        total = part[k, cube - 1]
        for slot in range(cube - 1):
            total = total + landed[k, slot]
        return signal[0] * total + noise[0] * v

    def gather(k, w):
        gathered[k, 0] = w
        for m in near_masks:
            remote(gathered.at[k, 0], gathered.at[k, m], sent.at[6 + k], gather_sem.at[k, m], gather_partner(m, 0)).start()
        remote(gathered.at[k, 0], gathered.at[k, cube], sent.at[6 + k], relay_sem.at[k], gather_partner(0, 1)).start()

    def take_gathered(k):
        split_into(0, gathered[k, 0])
        for m in reversed(near_masks):
            remote(gathered.at[k, 0], gathered.at[k, m], sent.at[6 + k], gather_sem.at[k, m], gather_partner(m, 0)).wait_recv()
            remote(gathered.at[k, m], gathered.at[k, cube + m], sent.at[6 + k], relay_sem.at[k], gather_partner(0, 1)).start()
            split_into(m, gathered[k, m])

    def take_relayed(k):
        await_bytes(gathered.at[k, cube : 2 * cube], relay_sem.at[k])
        each(cube, 2 * cube, lambda i: split_into(i, gathered[k, i]))

    lane = lax.broadcasted_iota(jnp.int32, (32, 128), 1)
    row_of = lax.broadcasted_iota(jnp.int32, (32, 128), 0)

    def tell(k, r, w):
        both = [jnp.sum(a, axis=1, keepdims=True) for a in (r * r, w * r)]
        met[k, 0:1] = sum(jnp.sum(jnp.where(lane == row_of + 32 * i, a, 0.0), axis=0, keepdims=True) for i, a in enumerate(both))
        for m, f in slots:
            at = f * cube + m
            remote(met.at[k, 0:1], met.at[k, at : at + 1], sent.at[8 + k], met_sem.at[k], gather_partner(m, f)).start()

    def pass_on(k):
        await_bytes(met.at[k, 1 : 2 * cube], met_sem.at[k])
        summed[k, cube - 1 : cube] = jnp.sum(met[k], axis=0, keepdims=True)
        for m in near_masks:
            at = cube - 1 - m
            remote(summed.at[k, cube - 1 : cube], summed.at[k, at : at + 1], sent.at[11 + k], summed_sem.at[k],
                   reduce_partner(m)).start()

    def hear(k):
        await_bytes(summed.at[k, 0 : cube - 1], summed_sem.at[k])
        total = jnp.sum(summed[k], axis=0, keepdims=True)
        return [jnp.sum(jnp.where(lane == row_of + 32 * i, total, 0.0), axis=1, keepdims=True) for i in range(2)]

    r = near_b[0]
    w = at_home(0, r)
    gather(0, w)
    tell(0, r, w)
    take_gathered(0)
    multiply(1)
    norm, curved = hear(0)
    alpha = norm / curved
    z = at_home(1, w)
    p, s = r, w
    r, w_next = r - alpha * s, w - alpha * z
    gather(1, w_next)
    tell(1, r, w_next)
    x = alpha * p
    take_gathered(1)
    multiply(2)
    w = w_next
    following, curved = hear(1)
    beta = following / norm
    norm, alpha = following, following / (curved - beta * following / alpha)
    p, s = r + beta * p, w + beta * s
    q = at_home(2, w)
    z = q + beta * z
    r, w = r - alpha * s, w - alpha * z
    tell(2, r, w)
    x = x + alpha * p
    pass_on(2)
    following, curved = hear(2)
    beta = following / norm
    alpha = following / (curved - beta * following / alpha)
    out_x[...] = x
    out_r[...] = r
    out_dx[...] = alpha * (r + beta * p)
    out_dr[...] = alpha * (w + beta * s)

    await_bytes(near.at[1 : 2 * cube], sent.at[0])
    await_bytes(far.at[0 : cube - 1], sent.at[1])
    await_bytes(near_b.at[1 : 2 * cube], sent.at[2])
    for k in range(3):
        await_bytes(landed.at[k], sent.at[3 + k])
        await_bytes(met.at[k, 1 : 2 * cube], sent.at[8 + k])
        await_bytes(summed.at[k, 0 : cube - 1], sent.at[11 + k])
    for k in range(2):
        await_bytes(gathered.at[k, 1 : 2 * cube], sent.at[6 + k])


def solution(mesh):
    rings = {1: 1, 4: 2, 16: 3}[mesh.shape["col"]]
    cube = 2**rings

    def body(points, lengthscale, signal, noise, targets, probe_bits):
        n = points.shape[1]
        depth, width, block = 2 * cube * n, 2 * n, (32, n)
        vmem = pl.BlockSpec(memory_space=pltpu.VMEM)
        smem = pl.BlockSpec(memory_space=pltpu.SMEM)
        hbm = pl.BlockSpec(memory_space=pl.ANY)
        x, r, dx, dr = pl.pallas_call(
            functools.partial(kernel, rings),
            out_shape=(jax.ShapeDtypeStruct(block, F32),) * 4,
            in_specs=[hbm, hbm, smem, smem, hbm, hbm],
            out_specs=(vmem,) * 4,
            scratch_shapes=[
                pltpu.VMEM((16, n), F32),
                pltpu.VMEM((1, 16), F32),
                pltpu.VMEM((1, n), F32),
                pltpu.VMEM((31, n), jnp.int32),
                pltpu.SemaphoreType.DMA((4,)),
                pltpu.VMEM((16, n), F32),
                pltpu.VMEM(block, F32),
                pltpu.VMEM((2 * cube, 16, n), F32),
                pltpu.VMEM((2 * cube, *block), F32),
                pltpu.VMEM((cube, 16, n), F32),
                pltpu.VMEM((depth, 128), BF16),
                pltpu.VMEM((cube // 2, 128, width), BF16),
                pltpu.VMEM((cube // 2, depth, width), BF16),
                pltpu.VMEM((cube // 2, depth, width), BF16),
                pltpu.VMEM((CHUNK, width), F32),
                pltpu.VMEM((CHUNK, width), F32),
                pltpu.VMEM((128, depth), BF16),
                pltpu.VMEM((3, cube, *block), F32),
                pltpu.VMEM((3, cube - 1, *block), F32),
                pltpu.VMEM((2, 2 * cube, *block), F32),
                pltpu.VMEM((3, 2 * cube, 128), F32),
                pltpu.VMEM((3, cube, 128), F32),
                pltpu.SemaphoreType.DMA((1,)),
                pltpu.SemaphoreType.DMA((2 * cube,)),
                pltpu.SemaphoreType.DMA((1,)),
                pltpu.SemaphoreType.DMA((3,)),
                pltpu.SemaphoreType.DMA((2, cube)),
                pltpu.SemaphoreType.DMA((2,)),
                pltpu.SemaphoreType.DMA((3,)),
                pltpu.SemaphoreType.DMA((3,)),
                pltpu.SemaphoreType.DMA((14,)),
            ],
            compiler_params=pltpu.CompilerParams(
                collective_id=0, has_side_effects=True,
                vmem_limit_bytes=60 * 1024 * 1024),
        )(points, lengthscale[None, :], signal, noise, targets[None, :], probe_bits)
        return x + dx, r - dr

    both = ("row", "col")
    placed = (P(None, both), P(), P(), P(), P(both), P(None, both))
    return jax.shard_map(body, mesh=mesh, in_specs=placed, out_specs=(P(None, both),) * 2, check_vma=False)
```

```python
import functools
import math

import jax
import jax.numpy as jnp
from jax import lax
from jax.experimental import pallas as pl
from jax.experimental.pallas import tpu as pltpu
from jax.sharding import PartitionSpec as P

F32 = jnp.float32
BF16 = jnp.bfloat16
MESH = pl.DeviceIdType.MESH
LN2 = math.log(2.0)
SPREAD = math.sqrt(5.0) / LN2
LINEAR = 3.0 / LN2
CONSTANT = 3.0 / LN2**2
CHUNK = 512


def pieces(x):
    first = x.astype(BF16).astype(F32)
    rest = x - first
    second = rest.astype(BF16).astype(F32)
    return first, second, (rest - second).astype(BF16).astype(F32)


def with_norms(x, before, after):
    parts = pieces(jnp.sum(x * x, axis=0, keepdims=True))
    row = lax.broadcasted_iota(jnp.int32, x.shape, 0)
    out = jnp.where((row >= after) & (row < after + 3), 1.0, 0.0)
    for i, part in enumerate(parts):
        out = jnp.where(row == before + i, part, out)
    return out


def left_operand(x):
    one, two, three = (-2.0 * p for p in pieces(x))
    return jnp.concatenate([one, one, two, two, one, three, with_norms(x, 0, 3), jnp.zeros_like(x)], axis=0)


def right_operand(x):
    one, two, three = pieces(x)
    return jnp.concatenate([one, two, one, two, three, one, with_norms(x, 3, 0), jnp.zeros_like(x)], axis=0)


def dot(a, b):
    return lax.dot_general(a, b, (((1,), (0,)), ((), ())), preferred_element_type=F32)


def flipped(v):
    return v + 1 - 2 * lax.rem(v, 2)


def turned(v):
    return lax.rem(v + 2 * lax.rem(v, 2) + 3, 4)


def kernel(rings, points, scales, signal, noise, targets, bits, out_x, out_r, out_dx, out_dr, out_alpha,
           points_here, scales_here, targets_here, bits_here, fetched, mine, mine_b, near, near_b, far, left, right, upper, lower, even, odd, vectors, part, landed, gathered,
           met, summed, near_b_sem, near_sem, far_sem, land_sem, gather_sem, relay_sem, met_sem, summed_sem, sent):
    n = points_here.shape[1]
    cube = 2**rings
    pairs = cube // 2
    width = 2 * n
    depth = 2 * cube * n
    chunks = depth // CHUNK
    row, col = lax.axis_index("row"), lax.axis_index("col")
    core = lax.rem(row, 2)
    place = [row // 2]
    for i in range(rings - 1):
        place.append(lax.rem(col // 4 ** (rings - 2 - i), 4))

    def device(places, core):
        c = 0
        for v in places[1:]:
            c = 4 * c + v
        return {"row": 2 * places[0] + core, "col": c}

    def gather_partner(mask, other):
        return device([flipped(v) if mask >> i & 1 else v for i, v in enumerate(place)], 1 - core if other else core)

    def reduce_partner(mask):
        return device([v + lax.rem(mask // 2**i, 2) * (turned(v) - v) for i, v in enumerate(place)], core)

    def remote(src, dst, send, recv, to):
        return pltpu.make_async_remote_copy(
            src_ref=src, dst_ref=dst, send_sem=send, recv_sem=recv, device_id=to, device_id_type=MESH)

    def await_bytes(ref, sem):
        pltpu.make_async_copy(ref, ref, sem).wait()

    def each(lo, hi, fn):
        def step(i, carry):
            fn(i)
            return carry
        lax.fori_loop(lo, hi, step, 0)

    near_masks = sorted(range(1, cube), key=lambda m: (-bin(m).count("1"), m))
    slots = [(m, f) for m in near_masks for f in range(2)] + [(0, 1)]

    barrier = pltpu.get_barrier_semaphore()
    for m, f in slots:
        pl.semaphore_signal(barrier, inc=1, device_id=gather_partner(m, f), device_id_type=MESH)
    for m in near_masks:
        pl.semaphore_signal(barrier, inc=1, device_id=reduce_partner(m), device_id_type=MESH)
    local = [pltpu.make_async_copy(src, dst, fetched.at[i])
             for i, (src, dst) in enumerate(((points, points_here), (scales, scales_here), (targets, targets_here), (bits, bits_here)))]
    for copy in local:
        copy.start()
    for copy in local:
        copy.wait()
    diagonal = lax.broadcasted_iota(jnp.int32, (16, 16), 0) == lax.broadcasted_iota(jnp.int32, (16, 16), 1)
    scale = jnp.sum(jnp.where(diagonal, scales_here[...], 0.0), axis=1, keepdims=True)
    x = points_here[...] / scale * SPREAD
    mine[...] = x
    near[0] = x
    far[cube - 1] = x
    mine_b[0:1, :] = targets_here[...]
    mine_b[1:32, :] = 2.0 * bits_here[...].astype(F32) - 1.0
    near_b[0] = mine_b[...]
    pl.semaphore_wait(barrier, len(slots) + len(near_masks))

    def send_near(m, f):
        return remote(mine, near.at[f * cube + m], sent.at[0], near_sem.at[f * cube + m], gather_partner(m, f))

    for m in near_masks:
        remote(mine, far.at[cube - 1 - m], sent.at[1], far_sem.at[0], reduce_partner(m)).start()
    for m, f in slots:
        send_near(m, f).start()
    for m, f in slots:
        remote(mine_b, near_b.at[f * cube + m], sent.at[2], near_b_sem.at[0], gather_partner(m, f)).start()

    def split_into(slot, d):
        at = pl.ds(pl.multiple_of(slot * n, n), n)
        for i, piece in enumerate(pieces(d)):
            vectors[32 * i : 32 * i + 32, at] = piece.astype(BF16)

    def place_left(i):
        left[i * n : i * n + n, :] = jnp.transpose(left_operand(near[i])).astype(BF16)

    def place_right(i):
        right[i // 2, :, pl.ds(pl.multiple_of(lax.rem(i, 2) * n, n), n)] = right_operand(far[i]).astype(BF16)

    place_left(0)
    for m, f in reversed(slots):
        send_near(m, f).wait_recv()
        place_left(f * cube + m)
    await_bytes(far.at[0 : cube - 1], far_sem.at[0])
    each(0, cube, place_right)

    def distances(p, c):
        return dot(left[pl.ds(pl.multiple_of(c * CHUNK, CHUNK), CHUNK), :], right[p])

    def evaluate(buffer, p, c):
        for at in range(0, CHUNK, 32):
            u = jnp.maximum(buffer[at : at + 32, :], 1e-30)
            q = u * lax.rsqrt(u)
            value = ((q + LINEAR) * q + CONSTANT) * jnp.exp2(-math.log2(CONSTANT) - q)
            high = value.astype(BF16)
            to = pl.ds(pl.multiple_of(c * CHUNK + at, 32), 32)
            upper[p, to, :] = high
            lower[p, to, :] = (value - upper[p, to, :].astype(F32)).astype(BF16)

    def product(p, at):
        v = vectors[:, at]
        both = dot(v, upper[p, at, :]) + dot(v, lower[p, at, :])
        return both[0:32] + (both[32:64] + both[64:96])

    def send_parts(k, p, total):
        for j in range(2):
            slot = 2 * p + j
            part[k, slot] = total[:, j * n : j * n + n]

            if slot < cube - 1:
                remote(part.at[k, slot], landed.at[k, slot], sent.at[3 + k], land_sem.at[k],
                       reduce_partner(cube - 1 - slot)).start()

    vectors[96:128, :] = jnp.zeros((32, depth), BF16)
    even[...] = distances(0, 0)
    def step(t):
        p, i = t // (chunks // 2), lax.rem(t, chunks // 2)
        odd[...] = distances(p, 2 * i + 1)
        evaluate(even, p, 2 * i)
        even[...] = distances(jnp.minimum(p + (2 * i + 2) // chunks, pairs - 1), lax.rem(2 * i + 2, chunks))
        evaluate(odd, p, 2 * i + 1)

    each(0, pairs * chunks // 2, step)
    await_bytes(near_b.at[1 : 2 * cube], near_b_sem.at[0])
    each(0, 2 * cube, lambda i: split_into(i, near_b[i]))

    def multiply(k):
        for p in range(pairs):
            send_parts(k, p, product(p, pl.ds(0, depth)))

    def at_home(k, v):
        await_bytes(landed.at[k], land_sem.at[k])
        total = part[k, cube - 1]
        for slot in range(cube - 1):
            total = total + landed[k, slot]
        return signal[0] * total + noise[0] * v

    def gather(k, w):
        gathered[k, 0] = w
        for m in near_masks:
            remote(gathered.at[k, 0], gathered.at[k, m], sent.at[6 + k], gather_sem.at[k, m], gather_partner(m, 0)).start()
        remote(gathered.at[k, 0], gathered.at[k, cube], sent.at[6 + k], relay_sem.at[k], gather_partner(0, 1)).start()

    def take_gathered(k):
        split_into(0, gathered[k, 0])
        for m in reversed(near_masks):
            remote(gathered.at[k, 0], gathered.at[k, m], sent.at[6 + k], gather_sem.at[k, m], gather_partner(m, 0)).wait_recv()
            remote(gathered.at[k, m], gathered.at[k, cube + m], sent.at[6 + k], relay_sem.at[k], gather_partner(0, 1)).start()
            split_into(m, gathered[k, m])

    def take_relayed(k):
        await_bytes(gathered.at[k, cube : 2 * cube], relay_sem.at[k])
        each(cube, 2 * cube, lambda i: split_into(i, gathered[k, i]))

    lane = lax.broadcasted_iota(jnp.int32, (32, 128), 1)
    row_of = lax.broadcasted_iota(jnp.int32, (32, 128), 0)

    def tell(k, r, w):
        both = [jnp.sum(a, axis=1, keepdims=True) for a in (r * r, w * r)]
        met[k, 0:1] = sum(jnp.sum(jnp.where(lane == row_of + 32 * i, a, 0.0), axis=0, keepdims=True) for i, a in enumerate(both))
        for m, f in slots:
            at = f * cube + m
            remote(met.at[k, 0:1], met.at[k, at : at + 1], sent.at[8 + k], met_sem.at[k], gather_partner(m, f)).start()

    def pass_on(k):
        await_bytes(met.at[k, 1 : 2 * cube], met_sem.at[k])
        summed[k, cube - 1 : cube] = jnp.sum(met[k], axis=0, keepdims=True)
        for m in near_masks:
            at = cube - 1 - m
            remote(summed.at[k, cube - 1 : cube], summed.at[k, at : at + 1], sent.at[11 + k], summed_sem.at[k],
                   reduce_partner(m)).start()

    def hear(k):
        await_bytes(summed.at[k, 0 : cube - 1], summed_sem.at[k])
        total = jnp.sum(summed[k], axis=0, keepdims=True)
        return [jnp.sum(jnp.where(lane == row_of + 32 * i, total, 0.0), axis=1, keepdims=True) for i in range(2)]

    multiply(0)
    r = near_b[0]
    w = at_home(0, r)
    gather(0, w)
    tell(0, r, w)
    take_gathered(0)
    take_relayed(0)
    pass_on(0)
    multiply(1)
    norm, curved = hear(0)
    alpha = norm / curved
    z = at_home(1, w)
    p, s = r, w
    r, w_next = r - alpha * s, w - alpha * z
    gather(1, w_next)
    tell(1, r, w_next)
    x = alpha * p
    take_gathered(1)
    take_relayed(1)
    pass_on(1)
    multiply(2)
    w = w_next
    following, curved = hear(1)
    beta = following / norm
    norm, alpha = following, following / (curved - beta * following / alpha)
    p, s = r + beta * p, w + beta * s
    q = at_home(2, w)
    z = q + beta * z
    r, w = r - alpha * s, w - alpha * z
    tell(2, r, w)
    x = x + alpha * p
    pass_on(2)
    following, curved = hear(2)
    beta = following / norm
    alpha = following / (curved - beta * following / alpha)
    out_x[...] = x
    out_r[...] = r
    out_dx[...] = r + beta * p
    out_dr[...] = w + beta * s
    out_alpha[...] = jnp.broadcast_to(alpha, r.shape)

    await_bytes(near.at[1 : 2 * cube], sent.at[0])
    await_bytes(far.at[0 : cube - 1], sent.at[1])
    await_bytes(near_b.at[1 : 2 * cube], sent.at[2])
    for k in range(3):
        await_bytes(landed.at[k], sent.at[3 + k])
        await_bytes(met.at[k, 1 : 2 * cube], sent.at[8 + k])
        await_bytes(summed.at[k, 0 : cube - 1], sent.at[11 + k])
    for k in range(2):
        await_bytes(gathered.at[k, 1 : 2 * cube], sent.at[6 + k])


def solution(mesh):
    rings = {1: 1, 4: 2, 16: 3}[mesh.shape["col"]]
    cube = 2**rings

    def body(points, lengthscale, signal, noise, targets, probe_bits):
        n = points.shape[1]
        depth, width, block = 2 * cube * n, 2 * n, (32, n)
        vmem = pl.BlockSpec(memory_space=pltpu.VMEM)
        smem = pl.BlockSpec(memory_space=pltpu.SMEM)
        hbm = pl.BlockSpec(memory_space=pl.ANY)
        x, r, dx, dr, alpha = pl.pallas_call(
            functools.partial(kernel, rings),
            out_shape=(jax.ShapeDtypeStruct(block, F32),) * 5,
            in_specs=[hbm, hbm, smem, smem, hbm, hbm],
            out_specs=(vmem,) * 5,
            scratch_shapes=[
                pltpu.VMEM((16, n), F32),
                pltpu.VMEM((1, 16), F32),
                pltpu.VMEM((1, n), F32),
                pltpu.VMEM((31, n), jnp.int32),
                pltpu.SemaphoreType.DMA((4,)),
                pltpu.VMEM((16, n), F32),
                pltpu.VMEM(block, F32),
                pltpu.VMEM((2 * cube, 16, n), F32),
                pltpu.VMEM((2 * cube, *block), F32),
                pltpu.VMEM((cube, 16, n), F32),
                pltpu.VMEM((depth, 128), BF16),
                pltpu.VMEM((cube // 2, 128, width), BF16),
                pltpu.VMEM((cube // 2, depth, width), BF16),
                pltpu.VMEM((cube // 2, depth, width), BF16),
                pltpu.VMEM((CHUNK, width), F32),
                pltpu.VMEM((CHUNK, width), F32),
                pltpu.VMEM((128, depth), BF16),
                pltpu.VMEM((3, cube, *block), F32),
                pltpu.VMEM((3, cube - 1, *block), F32),
                pltpu.VMEM((2, 2 * cube, *block), F32),
                pltpu.VMEM((3, 2 * cube, 128), F32),
                pltpu.VMEM((3, cube, 128), F32),
                pltpu.SemaphoreType.DMA((1,)),
                pltpu.SemaphoreType.DMA((2 * cube,)),
                pltpu.SemaphoreType.DMA((1,)),
                pltpu.SemaphoreType.DMA((3,)),
                pltpu.SemaphoreType.DMA((2, cube)),
                pltpu.SemaphoreType.DMA((2,)),
                pltpu.SemaphoreType.DMA((3,)),
                pltpu.SemaphoreType.DMA((3,)),
                pltpu.SemaphoreType.DMA((14,)),
            ],
            compiler_params=pltpu.CompilerParams(
                collective_id=0, has_side_effects=True,
                vmem_limit_bytes=60 * 1024 * 1024),
        )(points, lengthscale[None, :], signal, noise, targets[None, :], probe_bits)
        return x + alpha * dx, r - alpha * dr

    both = ("row", "col")
    placed = (P(None, both), P(), P(), P(), P(both), P(None, both))
    return jax.shard_map(body, mesh=mesh, in_specs=placed, out_specs=(P(None, both),) * 2, check_vma=False)
```

```python
import functools
import math

import jax
import jax.numpy as jnp
from jax import lax
from jax.experimental import pallas as pl
from jax.experimental.pallas import tpu as pltpu
from jax.sharding import PartitionSpec as P

F32 = jnp.float32
BF16 = jnp.bfloat16
MESH = pl.DeviceIdType.MESH
LN2 = math.log(2.0)
SPREAD = math.sqrt(5.0) / LN2
LINEAR = 3.0 / LN2
CONSTANT = 3.0 / LN2**2
CHUNK = 512


def pieces(x):
    first = x.astype(BF16).astype(F32)
    rest = x - first
    second = rest.astype(BF16).astype(F32)
    return first, second, (rest - second).astype(BF16).astype(F32)


def with_norms(x, before, after):
    parts = pieces(jnp.sum(x * x, axis=0, keepdims=True))
    row = lax.broadcasted_iota(jnp.int32, x.shape, 0)
    out = jnp.where((row >= after) & (row < after + 3), 1.0, 0.0)
    for i, part in enumerate(parts):
        out = jnp.where(row == before + i, part, out)
    return out


def left_operand(x):
    one, two, three = (-2.0 * p for p in pieces(x))
    return jnp.concatenate([one, one, two, two, one, three, with_norms(x, 0, 3), jnp.zeros_like(x)], axis=0)


def right_operand(x):
    one, two, three = pieces(x)
    return jnp.concatenate([one, two, one, two, three, one, with_norms(x, 3, 0), jnp.zeros_like(x)], axis=0)


def dot(a, b):
    return lax.dot_general(a, b, (((1,), (0,)), ((), ())), preferred_element_type=F32)


def flipped(v):
    return v + 1 - 2 * lax.rem(v, 2)


def turned(v):
    return lax.rem(v + 2 * lax.rem(v, 2) + 3, 4)


def kernel(rings, points, scales, signal, noise, targets, bits, out_x, out_r, out_dx, out_dr, out_alpha,
           points_here, scales_here, targets_here, bits_here, fetched, mine, mine_b, near, near_b, far, left, right, upper, lower, vectors, part, landed, gathered,
           met, summed, near_b_sem, near_sem, far_sem, land_sem, gather_sem, relay_sem, met_sem, summed_sem, sent):
    n = points_here.shape[1]
    cube = 2**rings
    pairs = cube // 2
    width = 2 * n
    depth = 2 * cube * n
    chunks = depth // CHUNK
    row, col = lax.axis_index("row"), lax.axis_index("col")
    core = lax.rem(row, 2)
    place = [row // 2]
    for i in range(rings - 1):
        place.append(lax.rem(col // 4 ** (rings - 2 - i), 4))

    def device(places, core):
        c = 0
        for v in places[1:]:
            c = 4 * c + v
        return {"row": 2 * places[0] + core, "col": c}

    def gather_partner(mask, other):
        return device([flipped(v) if mask >> i & 1 else v for i, v in enumerate(place)], 1 - core if other else core)

    def reduce_partner(mask):
        return device([v + lax.rem(mask // 2**i, 2) * (turned(v) - v) for i, v in enumerate(place)], core)

    def remote(src, dst, send, recv, to):
        return pltpu.make_async_remote_copy(
            src_ref=src, dst_ref=dst, send_sem=send, recv_sem=recv, device_id=to, device_id_type=MESH)

    def await_bytes(ref, sem):
        pltpu.make_async_copy(ref, ref, sem).wait()

    def each(lo, hi, fn):
        def step(i, carry):
            fn(i)
            return carry
        lax.fori_loop(lo, hi, step, 0)

    near_masks = sorted(range(1, cube), key=lambda m: (-bin(m).count("1"), m))
    slots = [(m, f) for m in near_masks for f in range(2)] + [(0, 1)]

    barrier = pltpu.get_barrier_semaphore()
    for m, f in slots:
        pl.semaphore_signal(barrier, inc=1, device_id=gather_partner(m, f), device_id_type=MESH)
    for m in near_masks:
        pl.semaphore_signal(barrier, inc=1, device_id=reduce_partner(m), device_id_type=MESH)
    local = [pltpu.make_async_copy(src, dst, fetched.at[i])
             for i, (src, dst) in enumerate(((points, points_here), (scales, scales_here), (targets, targets_here), (bits, bits_here)))]
    for copy in local:
        copy.start()
    for copy in local:
        copy.wait()
    diagonal = lax.broadcasted_iota(jnp.int32, (16, 16), 0) == lax.broadcasted_iota(jnp.int32, (16, 16), 1)
    scale = jnp.sum(jnp.where(diagonal, scales_here[...], 0.0), axis=1, keepdims=True)
    x = points_here[...] / scale * SPREAD
    mine[...] = x
    near[0] = x
    far[cube - 1] = x
    mine_b[0:1, :] = targets_here[...]
    mine_b[1:32, :] = 2.0 * bits_here[...].astype(F32) - 1.0
    near_b[0] = mine_b[...]
    pl.semaphore_wait(barrier, len(slots) + len(near_masks))

    def send_near(m, f):
        return remote(mine, near.at[f * cube + m], sent.at[0], near_sem.at[f * cube + m], gather_partner(m, f))

    for m in near_masks:
        remote(mine, far.at[cube - 1 - m], sent.at[1], far_sem.at[0], reduce_partner(m)).start()
    for m, f in slots:
        send_near(m, f).start()
    for m, f in slots:
        remote(mine_b, near_b.at[f * cube + m], sent.at[2], near_b_sem.at[0], gather_partner(m, f)).start()

    def split_into(slot, d):
        at = pl.ds(pl.multiple_of(slot * n, n), n)
        for i, piece in enumerate(pieces(d)):
            vectors[32 * i : 32 * i + 32, at] = piece.astype(BF16)

    def place_left(i):
        left[i * n : i * n + n, :] = jnp.transpose(left_operand(near[i])).astype(BF16)

    def place_right(i):
        right[i // 2, :, pl.ds(pl.multiple_of(lax.rem(i, 2) * n, n), n)] = right_operand(far[i]).astype(BF16)

    place_left(0)
    for m, f in reversed(slots):
        send_near(m, f).wait_recv()
        place_left(f * cube + m)
    await_bytes(far.at[0 : cube - 1], far_sem.at[0])
    each(0, cube, place_right)

    def distances(p, c):
        return dot(left[pl.ds(pl.multiple_of(c * CHUNK, CHUNK), CHUNK), :], right[p])

    def evaluate(buffer, p, c):
        for at in range(0, CHUNK, 32):
            u = jnp.maximum(buffer[at : at + 32, :], 1e-30)
            q = u * lax.rsqrt(u)
            value = ((q + LINEAR) * q + CONSTANT) * jnp.exp2(-math.log2(CONSTANT) - q)
            high = value.astype(BF16)
            to = pl.ds(pl.multiple_of(c * CHUNK + at, 32), 32)
            upper[p, to, :] = high
            lower[p, to, :] = (value - upper[p, to, :].astype(F32)).astype(BF16)

    def product(p, at):
        v = vectors[:, at]
        both = dot(v, upper[p, at, :]) + dot(v, lower[p, at, :])
        return both[0:32] + (both[32:64] + both[64:96])

    def send_parts(k, p, total):
        for j in range(2):
            slot = 2 * p + j
            part[k, slot] = total[:, j * n : j * n + n]

            def send():
                remote(part.at[k, slot], landed.at[k, slot], sent.at[3 + k], land_sem.at[k],
                       reduce_partner(cube - 1 - slot)).start()

            if isinstance(p, int):
                if slot < cube - 1:
                    send()
            elif j == 0:
                send()
            else:
                pl.when(p < pairs - 1)(send)

    vectors[96:128, :] = jnp.zeros((32, depth), BF16)
    def step(t):
        for j in range(4):
            c = t * 4 + j
            evaluate(distances(c // chunks, lax.rem(c, chunks)), c // chunks, lax.rem(c, chunks))

    each(0, pairs * chunks // 4, step)
    await_bytes(near_b.at[1 : 2 * cube], near_b_sem.at[0])
    each(0, 2 * cube, lambda i: split_into(i, near_b[i]))
    each(0, pairs, lambda p: send_parts(0, p, product(p, pl.ds(0, depth))))

    def multiply(k):
        take_relayed(k - 1)
        pass_on(k - 1)
        each(0, pairs, lambda p: send_parts(k, p, product(p, pl.ds(0, depth))))

    def at_home(k, v):
        await_bytes(landed.at[k], land_sem.at[k])
        total = part[k, cube - 1]
        for slot in range(cube - 1):
            total = total + landed[k, slot]
        return signal[0] * total + noise[0] * v

    def gather(k, w):
        gathered[k, 0] = w
        for m in near_masks:
            remote(gathered.at[k, 0], gathered.at[k, m], sent.at[6 + k], gather_sem.at[k, m], gather_partner(m, 0)).start()
        remote(gathered.at[k, 0], gathered.at[k, cube], sent.at[6 + k], relay_sem.at[k], gather_partner(0, 1)).start()

    def take_gathered(k):
        split_into(0, gathered[k, 0])
        for m in reversed(near_masks):
            remote(gathered.at[k, 0], gathered.at[k, m], sent.at[6 + k], gather_sem.at[k, m], gather_partner(m, 0)).wait_recv()
            remote(gathered.at[k, m], gathered.at[k, cube + m], sent.at[6 + k], relay_sem.at[k], gather_partner(0, 1)).start()
            split_into(m, gathered[k, m])

    def take_relayed(k):
        await_bytes(gathered.at[k, cube : 2 * cube], relay_sem.at[k])
        each(cube, 2 * cube, lambda i: split_into(i, gathered[k, i]))

    lane = lax.broadcasted_iota(jnp.int32, (32, 128), 1)
    row_of = lax.broadcasted_iota(jnp.int32, (32, 128), 0)

    def tell(k, r, w):
        both = [jnp.sum(a, axis=1, keepdims=True) for a in (r * r, w * r)]
        met[k, 0:1] = sum(jnp.sum(jnp.where(lane == row_of + 32 * i, a, 0.0), axis=0, keepdims=True) for i, a in enumerate(both))
        for m, f in slots:
            at = f * cube + m
            remote(met.at[k, 0:1], met.at[k, at : at + 1], sent.at[8 + k], met_sem.at[k], gather_partner(m, f)).start()

    def pass_on(k):
        await_bytes(met.at[k, 1 : 2 * cube], met_sem.at[k])
        summed[k, cube - 1 : cube] = jnp.sum(met[k], axis=0, keepdims=True)
        for m in near_masks:
            at = cube - 1 - m
            remote(summed.at[k, cube - 1 : cube], summed.at[k, at : at + 1], sent.at[11 + k], summed_sem.at[k],
                   reduce_partner(m)).start()

    def hear(k):
        await_bytes(summed.at[k, 0 : cube - 1], summed_sem.at[k])
        total = jnp.sum(summed[k], axis=0, keepdims=True)
        return [jnp.sum(jnp.where(lane == row_of + 32 * i, total, 0.0), axis=1, keepdims=True) for i in range(2)]

    r = near_b[0]
    w = at_home(0, r)
    gather(0, w)
    tell(0, r, w)
    take_gathered(0)
    multiply(1)
    norm, curved = hear(0)
    alpha = norm / curved
    z = at_home(1, w)
    p, s = r, w
    r, w_next = r - alpha * s, w - alpha * z
    gather(1, w_next)
    tell(1, r, w_next)
    x = alpha * p
    take_gathered(1)
    multiply(2)
    w = w_next
    following, curved = hear(1)
    beta = following / norm
    norm, alpha = following, following / (curved - beta * following / alpha)
    p, s = r + beta * p, w + beta * s
    q = at_home(2, w)
    z = q + beta * z
    r, w = r - alpha * s, w - alpha * z
    tell(2, r, w)
    x = x + alpha * p
    pass_on(2)
    following, curved = hear(2)
    beta = following / norm
    alpha = following / (curved - beta * following / alpha)
    out_x[...] = x
    out_r[...] = r
    out_dx[...] = r + beta * p
    out_dr[...] = w + beta * s
    out_alpha[...] = jnp.broadcast_to(alpha, r.shape)

    await_bytes(near.at[1 : 2 * cube], sent.at[0])
    await_bytes(far.at[0 : cube - 1], sent.at[1])
    await_bytes(near_b.at[1 : 2 * cube], sent.at[2])
    for k in range(3):
        await_bytes(landed.at[k], sent.at[3 + k])
        await_bytes(met.at[k, 1 : 2 * cube], sent.at[8 + k])
        await_bytes(summed.at[k, 0 : cube - 1], sent.at[11 + k])
    for k in range(2):
        await_bytes(gathered.at[k, 1 : 2 * cube], sent.at[6 + k])


def solution(mesh):
    rings = {1: 1, 4: 2, 16: 3}[mesh.shape["col"]]
    cube = 2**rings

    def body(points, lengthscale, signal, noise, targets, probe_bits):
        n = points.shape[1]
        depth, width, block = 2 * cube * n, 2 * n, (32, n)
        vmem = pl.BlockSpec(memory_space=pltpu.VMEM)
        smem = pl.BlockSpec(memory_space=pltpu.SMEM)
        hbm = pl.BlockSpec(memory_space=pl.ANY)
        x, r, dx, dr, alpha = pl.pallas_call(
            functools.partial(kernel, rings),
            out_shape=(jax.ShapeDtypeStruct(block, F32),) * 5,
            in_specs=[hbm, hbm, smem, smem, hbm, hbm],
            out_specs=(vmem,) * 5,
            scratch_shapes=[
                pltpu.VMEM((16, n), F32),
                pltpu.VMEM((1, 16), F32),
                pltpu.VMEM((1, n), F32),
                pltpu.VMEM((31, n), jnp.int32),
                pltpu.SemaphoreType.DMA((4,)),
                pltpu.VMEM((16, n), F32),
                pltpu.VMEM(block, F32),
                pltpu.VMEM((2 * cube, 16, n), F32),
                pltpu.VMEM((2 * cube, *block), F32),
                pltpu.VMEM((cube, 16, n), F32),
                pltpu.VMEM((depth, 128), BF16),
                pltpu.VMEM((cube // 2, 128, width), BF16),
                pltpu.VMEM((cube // 2, depth, width), BF16),
                pltpu.VMEM((cube // 2, depth, width), BF16),
                pltpu.VMEM((128, depth), BF16),
                pltpu.VMEM((3, cube, *block), F32),
                pltpu.VMEM((3, cube - 1, *block), F32),
                pltpu.VMEM((2, 2 * cube, *block), F32),
                pltpu.VMEM((3, 2 * cube, 128), F32),
                pltpu.VMEM((3, cube, 128), F32),
                pltpu.SemaphoreType.DMA((1,)),
                pltpu.SemaphoreType.DMA((2 * cube,)),
                pltpu.SemaphoreType.DMA((1,)),
                pltpu.SemaphoreType.DMA((3,)),
                pltpu.SemaphoreType.DMA((2, cube)),
                pltpu.SemaphoreType.DMA((2,)),
                pltpu.SemaphoreType.DMA((3,)),
                pltpu.SemaphoreType.DMA((3,)),
                pltpu.SemaphoreType.DMA((14,)),
            ],
            compiler_params=pltpu.CompilerParams(
                collective_id=0, has_side_effects=True,
                vmem_limit_bytes=60 * 1024 * 1024),
        )(points, lengthscale[None, :], signal, noise, targets[None, :], probe_bits)
        return x + alpha * dx, r - alpha * dr

    both = ("row", "col")
    placed = (P(None, both), P(), P(), P(), P(both), P(None, both))
    return jax.shard_map(body, mesh=mesh, in_specs=placed, out_specs=(P(None, both),) * 2, check_vma=False)
```

```python
import functools
import math

import jax
import jax.numpy as jnp
from jax import lax
from jax.experimental import pallas as pl
from jax.experimental.pallas import tpu as pltpu
from jax.sharding import PartitionSpec as P

F32 = jnp.float32
BF16 = jnp.bfloat16
MESH = pl.DeviceIdType.MESH
LN2 = math.log(2.0)
SPREAD = math.sqrt(5.0) / LN2
LINEAR = 3.0 / LN2
CONSTANT = 3.0 / LN2**2
CHUNK = 1024


def pieces(x):
    first = x.astype(BF16).astype(F32)
    rest = x - first
    second = rest.astype(BF16).astype(F32)
    return first, second, (rest - second).astype(BF16).astype(F32)


def with_norms(x, before, after):
    parts = pieces(jnp.sum(x * x, axis=0, keepdims=True))
    row = lax.broadcasted_iota(jnp.int32, x.shape, 0)
    out = jnp.where((row >= after) & (row < after + 3), 1.0, 0.0)
    for i, part in enumerate(parts):
        out = jnp.where(row == before + i, part, out)
    return out


def left_operand(x):
    one, two, three = (-2.0 * p for p in pieces(x))
    return jnp.concatenate([one, one, two, two, one, three, with_norms(x, 0, 3), jnp.zeros_like(x)], axis=0)


def right_operand(x):
    one, two, three = pieces(x)
    return jnp.concatenate([one, two, one, two, three, one, with_norms(x, 3, 0), jnp.zeros_like(x)], axis=0)


def dot(a, b):
    return lax.dot_general(a, b, (((1,), (0,)), ((), ())), preferred_element_type=F32)


def flipped(v):
    return v + 1 - 2 * lax.rem(v, 2)


def turned(v):
    return lax.rem(v + 2 * lax.rem(v, 2) + 3, 4)


def kernel(rings, points, scales, signal, noise, targets, bits, out_x, out_r, out_dx, out_dr, out_alpha,
           points_here, scales_here, targets_here, bits_here, fetched, mine, mine_b, near, near_b, far, left, right, upper, lower, vectors, part, landed, gathered,
           met, summed, near_b_sem, near_sem, far_sem, land_sem, gather_sem, relay_sem, met_sem, summed_sem, sent):
    n = points_here.shape[1]
    cube = 2**rings
    pairs = cube // 2
    width = 2 * n
    depth = 2 * cube * n
    chunks = depth // CHUNK
    row, col = lax.axis_index("row"), lax.axis_index("col")
    core = lax.rem(row, 2)
    place = [row // 2]
    for i in range(rings - 1):
        place.append(lax.rem(col // 4 ** (rings - 2 - i), 4))

    def device(places, core):
        c = 0
        for v in places[1:]:
            c = 4 * c + v
        return {"row": 2 * places[0] + core, "col": c}

    def gather_partner(mask, other):
        return device([flipped(v) if mask >> i & 1 else v for i, v in enumerate(place)], 1 - core if other else core)

    def reduce_partner(mask):
        return device([v + lax.rem(mask // 2**i, 2) * (turned(v) - v) for i, v in enumerate(place)], core)

    def remote(src, dst, send, recv, to):
        return pltpu.make_async_remote_copy(
            src_ref=src, dst_ref=dst, send_sem=send, recv_sem=recv, device_id=to, device_id_type=MESH)

    def await_bytes(ref, sem):
        pltpu.make_async_copy(ref, ref, sem).wait()

    def each(lo, hi, fn):
        def step(i, carry):
            fn(i)
            return carry
        lax.fori_loop(lo, hi, step, 0)

    near_masks = sorted(range(1, cube), key=lambda m: (-bin(m).count("1"), m))
    slots = [(m, f) for m in near_masks for f in range(2)] + [(0, 1)]

    barrier = pltpu.get_barrier_semaphore()
    for m, f in slots:
        pl.semaphore_signal(barrier, inc=1, device_id=gather_partner(m, f), device_id_type=MESH)
    for m in near_masks:
        pl.semaphore_signal(barrier, inc=1, device_id=reduce_partner(m), device_id_type=MESH)
    local = [pltpu.make_async_copy(src, dst, fetched.at[i])
             for i, (src, dst) in enumerate(((points, points_here), (scales, scales_here), (targets, targets_here), (bits, bits_here)))]
    for copy in local:
        copy.start()
    for copy in local:
        copy.wait()
    diagonal = lax.broadcasted_iota(jnp.int32, (16, 16), 0) == lax.broadcasted_iota(jnp.int32, (16, 16), 1)
    scale = jnp.sum(jnp.where(diagonal, scales_here[...], 0.0), axis=1, keepdims=True)
    x = points_here[...] / scale * SPREAD
    mine[...] = x
    near[0] = x
    far[cube - 1] = x
    mine_b[0:1, :] = targets_here[...]
    mine_b[1:32, :] = 2.0 * bits_here[...].astype(F32) - 1.0
    near_b[0] = mine_b[...]
    pl.semaphore_wait(barrier, len(slots) + len(near_masks))

    def send_near(m, f):
        return remote(mine, near.at[f * cube + m], sent.at[0], near_sem.at[f * cube + m], gather_partner(m, f))

    for m in near_masks:
        remote(mine, far.at[cube - 1 - m], sent.at[1], far_sem.at[0], reduce_partner(m)).start()
    for m, f in slots:
        send_near(m, f).start()
    for m, f in slots:
        remote(mine_b, near_b.at[f * cube + m], sent.at[2], near_b_sem.at[0], gather_partner(m, f)).start()

    def split_into(slot, d):
        at = pl.ds(pl.multiple_of(slot * n, n), n)
        for i, piece in enumerate(pieces(d)):
            vectors[32 * i : 32 * i + 32, at] = piece.astype(BF16)

    def place_left(i):
        left[i * n : i * n + n, :] = jnp.transpose(left_operand(near[i])).astype(BF16)

    def place_right(i):
        right[i // 2, :, pl.ds(pl.multiple_of(lax.rem(i, 2) * n, n), n)] = right_operand(far[i]).astype(BF16)

    place_left(0)
    for m, f in reversed(slots):
        send_near(m, f).wait_recv()
        place_left(f * cube + m)
    await_bytes(far.at[0 : cube - 1], far_sem.at[0])
    each(0, cube, place_right)

    def distances(p, c):
        return dot(left[pl.ds(pl.multiple_of(c * CHUNK, CHUNK), CHUNK), :], right[p])

    def evaluate(buffer, p, c):
        for at in range(0, CHUNK, 32):
            u = jnp.maximum(buffer[at : at + 32, :], 1e-30)
            q = u * lax.rsqrt(u)
            value = ((q + LINEAR) * q + CONSTANT) * jnp.exp2(-math.log2(CONSTANT) - q)
            high = value.astype(BF16)
            to = pl.ds(pl.multiple_of(c * CHUNK + at, 32), 32)
            upper[p, to, :] = high
            lower[p, to, :] = (value - upper[p, to, :].astype(F32)).astype(BF16)

    def product(p, at):
        v = vectors[:, at]
        both = dot(v, upper[p, at, :]) + dot(v, lower[p, at, :])
        return both[0:32] + (both[32:64] + both[64:96])

    def send_parts(k, p, total):
        for j in range(2):
            slot = 2 * p + j
            part[k, slot] = total[:, j * n : j * n + n]

            def send():
                remote(part.at[k, slot], landed.at[k, slot], sent.at[3 + k], land_sem.at[k],
                       reduce_partner(cube - 1 - slot)).start()

            if isinstance(p, int):
                if slot < cube - 1:
                    send()
            elif j == 0:
                send()
            else:
                pl.when(p < pairs - 1)(send)

    vectors[96:128, :] = jnp.zeros((32, depth), BF16)
    def step(t):
        for j in range(2):
            c = t * 2 + j
            evaluate(distances(c // chunks, lax.rem(c, chunks)), c // chunks, lax.rem(c, chunks))

    each(0, pairs * chunks // 2, step)
    await_bytes(near_b.at[1 : 2 * cube], near_b_sem.at[0])
    each(0, 2 * cube, lambda i: split_into(i, near_b[i]))
    each(0, pairs, lambda p: send_parts(0, p, product(p, pl.ds(0, depth))))

    def multiply(k):
        take_relayed(k - 1)
        pass_on(k - 1)
        each(0, pairs, lambda p: send_parts(k, p, product(p, pl.ds(0, depth))))

    def at_home(k, v):
        await_bytes(landed.at[k], land_sem.at[k])
        total = part[k, cube - 1]
        for slot in range(cube - 1):
            total = total + landed[k, slot]
        return signal[0] * total + noise[0] * v

    def gather(k, w):
        gathered[k, 0] = w
        for m in near_masks:
            remote(gathered.at[k, 0], gathered.at[k, m], sent.at[6 + k], gather_sem.at[k, m], gather_partner(m, 0)).start()
        remote(gathered.at[k, 0], gathered.at[k, cube], sent.at[6 + k], relay_sem.at[k], gather_partner(0, 1)).start()

    def take_gathered(k):
        split_into(0, gathered[k, 0])
        for m in reversed(near_masks):
            remote(gathered.at[k, 0], gathered.at[k, m], sent.at[6 + k], gather_sem.at[k, m], gather_partner(m, 0)).wait_recv()
            remote(gathered.at[k, m], gathered.at[k, cube + m], sent.at[6 + k], relay_sem.at[k], gather_partner(0, 1)).start()
            split_into(m, gathered[k, m])

    def take_relayed(k):
        await_bytes(gathered.at[k, cube : 2 * cube], relay_sem.at[k])
        each(cube, 2 * cube, lambda i: split_into(i, gathered[k, i]))

    lane = lax.broadcasted_iota(jnp.int32, (32, 128), 1)
    row_of = lax.broadcasted_iota(jnp.int32, (32, 128), 0)

    def tell(k, r, w):
        both = [jnp.sum(a, axis=1, keepdims=True) for a in (r * r, w * r)]
        met[k, 0:1] = sum(jnp.sum(jnp.where(lane == row_of + 32 * i, a, 0.0), axis=0, keepdims=True) for i, a in enumerate(both))
        for m, f in slots:
            at = f * cube + m
            remote(met.at[k, 0:1], met.at[k, at : at + 1], sent.at[8 + k], met_sem.at[k], gather_partner(m, f)).start()

    def pass_on(k):
        await_bytes(met.at[k, 1 : 2 * cube], met_sem.at[k])
        summed[k, cube - 1 : cube] = jnp.sum(met[k], axis=0, keepdims=True)
        for m in near_masks:
            at = cube - 1 - m
            remote(summed.at[k, cube - 1 : cube], summed.at[k, at : at + 1], sent.at[11 + k], summed_sem.at[k],
                   reduce_partner(m)).start()

    def hear(k):
        await_bytes(summed.at[k, 0 : cube - 1], summed_sem.at[k])
        total = jnp.sum(summed[k], axis=0, keepdims=True)
        return [jnp.sum(jnp.where(lane == row_of + 32 * i, total, 0.0), axis=1, keepdims=True) for i in range(2)]

    r = near_b[0]
    w = at_home(0, r)
    gather(0, w)
    tell(0, r, w)
    take_gathered(0)
    multiply(1)
    norm, curved = hear(0)
    alpha = norm / curved
    z = at_home(1, w)
    p, s = r, w
    r, w_next = r - alpha * s, w - alpha * z
    gather(1, w_next)
    tell(1, r, w_next)
    x = alpha * p
    take_gathered(1)
    multiply(2)
    w = w_next
    following, curved = hear(1)
    beta = following / norm
    norm, alpha = following, following / (curved - beta * following / alpha)
    p, s = r + beta * p, w + beta * s
    q = at_home(2, w)
    z = q + beta * z
    r, w = r - alpha * s, w - alpha * z
    tell(2, r, w)
    x = x + alpha * p
    pass_on(2)
    following, curved = hear(2)
    beta = following / norm
    alpha = following / (curved - beta * following / alpha)
    out_x[...] = x
    out_r[...] = r
    out_dx[...] = r + beta * p
    out_dr[...] = w + beta * s
    out_alpha[...] = jnp.broadcast_to(alpha, r.shape)

    await_bytes(near.at[1 : 2 * cube], sent.at[0])
    await_bytes(far.at[0 : cube - 1], sent.at[1])
    await_bytes(near_b.at[1 : 2 * cube], sent.at[2])
    for k in range(3):
        await_bytes(landed.at[k], sent.at[3 + k])
        await_bytes(met.at[k, 1 : 2 * cube], sent.at[8 + k])
        await_bytes(summed.at[k, 0 : cube - 1], sent.at[11 + k])
    for k in range(2):
        await_bytes(gathered.at[k, 1 : 2 * cube], sent.at[6 + k])


def solution(mesh):
    rings = {1: 1, 4: 2, 16: 3}[mesh.shape["col"]]
    cube = 2**rings

    def body(points, lengthscale, signal, noise, targets, probe_bits):
        n = points.shape[1]
        depth, width, block = 2 * cube * n, 2 * n, (32, n)
        vmem = pl.BlockSpec(memory_space=pltpu.VMEM)
        smem = pl.BlockSpec(memory_space=pltpu.SMEM)
        hbm = pl.BlockSpec(memory_space=pl.ANY)
        x, r, dx, dr, alpha = pl.pallas_call(
            functools.partial(kernel, rings),
            out_shape=(jax.ShapeDtypeStruct(block, F32),) * 5,
            in_specs=[hbm, hbm, smem, smem, hbm, hbm],
            out_specs=(vmem,) * 5,
            scratch_shapes=[
                pltpu.VMEM((16, n), F32),
                pltpu.VMEM((1, 16), F32),
                pltpu.VMEM((1, n), F32),
                pltpu.VMEM((31, n), jnp.int32),
                pltpu.SemaphoreType.DMA((4,)),
                pltpu.VMEM((16, n), F32),
                pltpu.VMEM(block, F32),
                pltpu.VMEM((2 * cube, 16, n), F32),
                pltpu.VMEM((2 * cube, *block), F32),
                pltpu.VMEM((cube, 16, n), F32),
                pltpu.VMEM((depth, 128), BF16),
                pltpu.VMEM((cube // 2, 128, width), BF16),
                pltpu.VMEM((cube // 2, depth, width), BF16),
                pltpu.VMEM((cube // 2, depth, width), BF16),
                pltpu.VMEM((128, depth), BF16),
                pltpu.VMEM((3, cube, *block), F32),
                pltpu.VMEM((3, cube - 1, *block), F32),
                pltpu.VMEM((2, 2 * cube, *block), F32),
                pltpu.VMEM((3, 2 * cube, 128), F32),
                pltpu.VMEM((3, cube, 128), F32),
                pltpu.SemaphoreType.DMA((1,)),
                pltpu.SemaphoreType.DMA((2 * cube,)),
                pltpu.SemaphoreType.DMA((1,)),
                pltpu.SemaphoreType.DMA((3,)),
                pltpu.SemaphoreType.DMA((2, cube)),
                pltpu.SemaphoreType.DMA((2,)),
                pltpu.SemaphoreType.DMA((3,)),
                pltpu.SemaphoreType.DMA((3,)),
                pltpu.SemaphoreType.DMA((14,)),
            ],
            compiler_params=pltpu.CompilerParams(
                collective_id=0, has_side_effects=True,
                vmem_limit_bytes=60 * 1024 * 1024),
        )(points, lengthscale[None, :], signal, noise, targets[None, :], probe_bits)
        return x + alpha * dx, r - alpha * dr

    both = ("row", "col")
    placed = (P(None, both), P(), P(), P(), P(both), P(None, both))
    return jax.shard_map(body, mesh=mesh, in_specs=placed, out_specs=(P(None, both),) * 2, check_vma=False)
```

```python
import functools
import math

import jax
import jax.numpy as jnp
from jax import lax
from jax.experimental import pallas as pl
from jax.experimental.pallas import tpu as pltpu
from jax.sharding import PartitionSpec as P

F32 = jnp.float32
BF16 = jnp.bfloat16
MESH = pl.DeviceIdType.MESH
LN2 = math.log(2.0)
SPREAD = math.sqrt(5.0) / LN2
LINEAR = 3.0 / LN2
CONSTANT = 3.0 / LN2**2
CHUNK = 1024


def pieces(x):
    first = x.astype(BF16).astype(F32)
    rest = x - first
    second = rest.astype(BF16).astype(F32)
    return first, second, (rest - second).astype(BF16).astype(F32)


def with_norms(x, before, after):
    parts = pieces(jnp.sum(x * x, axis=0, keepdims=True))
    row = lax.broadcasted_iota(jnp.int32, x.shape, 0)
    out = jnp.where((row >= after) & (row < after + 3), 1.0, 0.0)
    for i, part in enumerate(parts):
        out = jnp.where(row == before + i, part, out)
    return out


def left_operand(x):
    one, two, three = (-2.0 * p for p in pieces(x))
    return jnp.concatenate([one, one, two, two, one, three, with_norms(x, 0, 3), jnp.zeros_like(x)], axis=0)


def right_operand(x):
    one, two, three = pieces(x)
    return jnp.concatenate([one, two, one, two, three, one, with_norms(x, 3, 0), jnp.zeros_like(x)], axis=0)


def dot(a, b):
    return lax.dot_general(a, b, (((1,), (0,)), ((), ())), preferred_element_type=F32)


def flipped(v):
    return v + 1 - 2 * lax.rem(v, 2)


def turned(v):
    return lax.rem(v + 2 * lax.rem(v, 2) + 3, 4)


def kernel(rings, points, scales, signal, noise, targets, bits, out_x, out_r, out_dx, out_dr, out_alpha,
           points_here, scales_here, targets_here, bits_here, fetched, mine, mine_b, near, near_b, far, left, right, upper, lower, vectors, part, landed, gathered,
           met, summed, near_b_sem, near_sem, far_sem, land_sem, gather_sem, relay_sem, met_sem, summed_sem, sent):
    n = points_here.shape[1]
    cube = 2**rings
    pairs = cube // 2
    width = 2 * n
    depth = 2 * cube * n
    chunks = depth // CHUNK
    row, col = lax.axis_index("row"), lax.axis_index("col")
    core = lax.rem(row, 2)
    place = [row // 2]
    for i in range(rings - 1):
        place.append(lax.rem(col // 4 ** (rings - 2 - i), 4))

    def device(places, core):
        c = 0
        for v in places[1:]:
            c = 4 * c + v
        return {"row": 2 * places[0] + core, "col": c}

    def gather_partner(mask, other):
        return device([flipped(v) if mask >> i & 1 else v for i, v in enumerate(place)], 1 - core if other else core)

    def reduce_partner(mask):
        return device([v + lax.rem(mask // 2**i, 2) * (turned(v) - v) for i, v in enumerate(place)], core)

    def remote(src, dst, send, recv, to):
        return pltpu.make_async_remote_copy(
            src_ref=src, dst_ref=dst, send_sem=send, recv_sem=recv, device_id=to, device_id_type=MESH)

    def await_bytes(ref, sem):
        pltpu.make_async_copy(ref, ref, sem).wait()

    def each(lo, hi, fn):
        def step(i, carry):
            fn(i)
            return carry
        lax.fori_loop(lo, hi, step, 0)

    near_masks = sorted(range(1, cube), key=lambda m: (-bin(m).count("1"), m))
    slots = [(m, f) for m in near_masks for f in range(2)] + [(0, 1)]

    barrier = pltpu.get_barrier_semaphore()
    for m, f in slots:
        pl.semaphore_signal(barrier, inc=1, device_id=gather_partner(m, f), device_id_type=MESH)
    for m in near_masks:
        pl.semaphore_signal(barrier, inc=1, device_id=reduce_partner(m), device_id_type=MESH)
    local = [pltpu.make_async_copy(src, dst, fetched.at[i])
             for i, (src, dst) in enumerate(((points, points_here), (scales, scales_here), (targets, targets_here), (bits, bits_here)))]
    for copy in local:
        copy.start()
    for copy in local:
        copy.wait()
    diagonal = lax.broadcasted_iota(jnp.int32, (16, 16), 0) == lax.broadcasted_iota(jnp.int32, (16, 16), 1)
    scale = jnp.sum(jnp.where(diagonal, scales_here[...], 0.0), axis=1, keepdims=True)
    x = points_here[...] / scale * SPREAD
    mine[...] = x
    near[0] = x
    far[cube - 1] = x
    mine_b[0:1, :] = targets_here[...]
    mine_b[1:32, :] = 2.0 * bits_here[...].astype(F32) - 1.0
    near_b[0] = mine_b[...]
    pl.semaphore_wait(barrier, len(slots) + len(near_masks))

    def send_near(m, f):
        return remote(mine, near.at[f * cube + m], sent.at[0], near_sem.at[f * cube + m], gather_partner(m, f))

    for m in near_masks:
        remote(mine, far.at[cube - 1 - m], sent.at[1], far_sem.at[0], reduce_partner(m)).start()
    for m, f in slots:
        send_near(m, f).start()
    for m, f in slots:
        remote(mine_b, near_b.at[f * cube + m], sent.at[2], near_b_sem.at[0], gather_partner(m, f)).start()

    def split_into(slot, d):
        at = pl.ds(slot * n if isinstance(slot, int) else pl.multiple_of(slot * n, n), n)
        high = d.astype(BF16)
        vectors[0:32, at] = high
        vectors[32:64, at] = (d - high.astype(F32)).astype(BF16)

    def place_left(i):
        left[i * n : i * n + n, :] = jnp.transpose(left_operand(near[i])).astype(BF16)

    def place_right(i):
        right[i // 2, :, pl.ds(pl.multiple_of(lax.rem(i, 2) * n, n), n)] = right_operand(far[i]).astype(BF16)

    place_left(0)
    await_bytes(far.at[0 : cube - 1], far_sem.at[0])
    each(0, cube, place_right)
    for m, f in reversed(slots):
        send_near(m, f).wait_recv()
        place_left(f * cube + m)

    def distances(p, c):
        return dot(left[pl.ds(pl.multiple_of(c * CHUNK, CHUNK), CHUNK), :], right[p])

    def evaluate(buffer, p, c):
        for at in range(0, CHUNK, 32):
            u = jnp.maximum(buffer[at : at + 32, :], 1e-30)
            q = u * lax.rsqrt(u)
            value = ((q + LINEAR) * q + CONSTANT) * jnp.exp2(-math.log2(CONSTANT) - q)
            high = value.astype(BF16)
            to = pl.ds(pl.multiple_of(c * CHUNK + at, 32), 32)
            upper[p, to, :] = high
            lower[p, to, :] = (value - upper[p, to, :].astype(F32)).astype(BF16)

    def product(p, at):
        v = vectors[:, at]
        both = dot(v, upper[p, at, :]) + dot(v, lower[p, at, :])
        return both[0:32] + both[32:64]

    def send_parts(k, p, total):
        for j in range(2):
            slot = 2 * p + j
            part[k, slot] = total[:, j * n : j * n + n]

            def send():
                remote(part.at[k, slot], landed.at[k, slot], sent.at[3 + k], land_sem.at[k],
                       reduce_partner(cube - 1 - slot)).start()

            if isinstance(p, int):
                if slot < cube - 1:
                    send()
            elif j == 0:
                send()
            else:
                pl.when(p < pairs - 1)(send)

    vectors[64:128, :] = jnp.zeros((64, depth), BF16)
    def step(t):
        for j in range(2):
            c = t * 2 + j
            evaluate(distances(c // chunks, lax.rem(c, chunks)), c // chunks, lax.rem(c, chunks))

    each(0, pairs * chunks // 2, step)
    await_bytes(near_b.at[1 : 2 * cube], near_b_sem.at[0])
    each(0, 2 * cube, lambda i: split_into(i, near_b[i]))
    each(0, pairs, lambda p: send_parts(0, p, product(p, pl.ds(0, depth))))

    def multiply(k):
        take_relayed(k - 1)
        pass_on(k - 1)
        def go(i):
            for j in range(2):
                send_parts(k, 2 * i + j, product(2 * i + j, pl.ds(0, depth)))

        each(0, pairs // 2, go)

    def at_home(k, v):
        await_bytes(landed.at[k], land_sem.at[k])
        total = part[k, cube - 1]
        for slot in range(cube - 1):
            total = total + landed[k, slot]
        return signal[0] * total + noise[0] * v

    def gather(k, w):
        gathered[k, 0] = w
        for m in near_masks:
            remote(gathered.at[k, 0], gathered.at[k, m], sent.at[6 + k], gather_sem.at[k, m], gather_partner(m, 0)).start()
        remote(gathered.at[k, 0], gathered.at[k, cube], sent.at[6 + k], relay_sem.at[k, 0], gather_partner(0, 1)).start()

    def relay(k, m):
        return remote(gathered.at[k, m], gathered.at[k, cube + m], sent.at[6 + k], relay_sem.at[k, m], gather_partner(0, 1))

    def take_gathered(k):
        split_into(0, gathered[k, 0])
        for m in reversed(near_masks):
            remote(gathered.at[k, 0], gathered.at[k, m], sent.at[6 + k], gather_sem.at[k, m], gather_partner(m, 0)).wait_recv()
            relay(k, m).start()
        for m in near_masks:
            split_into(m, gathered[k, m])

    def take_relayed(k):
        for m in [0, *reversed(near_masks)]:
            relay(k, m).wait_recv()
            split_into(cube + m, gathered[k, cube + m])

    lane = lax.broadcasted_iota(jnp.int32, (32, 128), 1)
    row_of = lax.broadcasted_iota(jnp.int32, (32, 128), 0)

    def tell(k, r, w):
        both = [jnp.sum(a, axis=1, keepdims=True) for a in (r * r, w * r)]
        met[k, 0:1] = sum(jnp.sum(jnp.where(lane == row_of + 32 * i, a, 0.0), axis=0, keepdims=True) for i, a in enumerate(both))
        for m, f in slots:
            at = f * cube + m
            remote(met.at[k, 0:1], met.at[k, at : at + 1], sent.at[8 + k], met_sem.at[k], gather_partner(m, f)).start()

    def pass_on(k):
        await_bytes(met.at[k, 1 : 2 * cube], met_sem.at[k])
        summed[k, cube - 1 : cube] = jnp.sum(met[k], axis=0, keepdims=True)
        for m in near_masks:
            at = cube - 1 - m
            remote(summed.at[k, cube - 1 : cube], summed.at[k, at : at + 1], sent.at[11 + k], summed_sem.at[k],
                   reduce_partner(m)).start()

    def hear(k):
        await_bytes(summed.at[k, 0 : cube - 1], summed_sem.at[k])
        total = jnp.sum(summed[k], axis=0, keepdims=True)
        return [jnp.sum(jnp.where(lane == row_of + 32 * i, total, 0.0), axis=1, keepdims=True) for i in range(2)]

    r = near_b[0]
    w = at_home(0, r)
    gather(0, w)
    tell(0, r, w)
    take_gathered(0)
    multiply(1)
    norm, curved = hear(0)
    alpha = norm / curved
    z = at_home(1, w)
    p, s = r, w
    r, w_next = r - alpha * s, w - alpha * z
    gather(1, w_next)
    tell(1, r, w_next)
    x = alpha * p
    take_gathered(1)
    multiply(2)
    w = w_next
    following, curved = hear(1)
    beta = following / norm
    norm, alpha = following, following / (curved - beta * following / alpha)
    p, s = r + beta * p, w + beta * s
    q = at_home(2, w)
    z = q + beta * z
    r, w = r - alpha * s, w - alpha * z
    tell(2, r, w)
    x = x + alpha * p
    pass_on(2)
    following, curved = hear(2)
    beta = following / norm
    alpha = following / (curved - beta * following / alpha)
    out_x[...] = x
    out_r[...] = r
    out_dx[...] = r + beta * p
    out_dr[...] = w + beta * s
    out_alpha[...] = jnp.broadcast_to(alpha, r.shape)

    await_bytes(near.at[1 : 2 * cube], sent.at[0])
    await_bytes(far.at[0 : cube - 1], sent.at[1])
    await_bytes(near_b.at[1 : 2 * cube], sent.at[2])
    for k in range(3):
        await_bytes(landed.at[k], sent.at[3 + k])
        await_bytes(met.at[k, 1 : 2 * cube], sent.at[8 + k])
        await_bytes(summed.at[k, 0 : cube - 1], sent.at[11 + k])
    for k in range(2):
        await_bytes(gathered.at[k, 1 : 2 * cube], sent.at[6 + k])


def solution(mesh):
    rings = {1: 1, 4: 2, 16: 3}[mesh.shape["col"]]
    cube = 2**rings

    def body(points, lengthscale, signal, noise, targets, probe_bits):
        n = points.shape[1]
        depth, width, block = 2 * cube * n, 2 * n, (32, n)
        vmem = pl.BlockSpec(memory_space=pltpu.VMEM)
        smem = pl.BlockSpec(memory_space=pltpu.SMEM)
        hbm = pl.BlockSpec(memory_space=pl.ANY)
        x, r, dx, dr, alpha = pl.pallas_call(
            functools.partial(kernel, rings),
            out_shape=(jax.ShapeDtypeStruct(block, F32),) * 5,
            in_specs=[hbm, hbm, smem, smem, hbm, hbm],
            out_specs=(vmem,) * 5,
            scratch_shapes=[
                pltpu.VMEM((16, n), F32),
                pltpu.VMEM((1, 16), F32),
                pltpu.VMEM((1, n), F32),
                pltpu.VMEM((31, n), jnp.int32),
                pltpu.SemaphoreType.DMA((4,)),
                pltpu.VMEM((16, n), F32),
                pltpu.VMEM(block, F32),
                pltpu.VMEM((2 * cube, 16, n), F32),
                pltpu.VMEM((2 * cube, *block), F32),
                pltpu.VMEM((cube, 16, n), F32),
                pltpu.VMEM((depth, 128), BF16),
                pltpu.VMEM((cube // 2, 128, width), BF16),
                pltpu.VMEM((cube // 2, depth, width), BF16),
                pltpu.VMEM((cube // 2, depth, width), BF16),
                pltpu.VMEM((128, depth), BF16),
                pltpu.VMEM((3, cube, *block), F32),
                pltpu.VMEM((3, cube - 1, *block), F32),
                pltpu.VMEM((2, 2 * cube, *block), F32),
                pltpu.VMEM((3, 2 * cube, 128), F32),
                pltpu.VMEM((3, cube, 128), F32),
                pltpu.SemaphoreType.DMA((1,)),
                pltpu.SemaphoreType.DMA((2 * cube,)),
                pltpu.SemaphoreType.DMA((1,)),
                pltpu.SemaphoreType.DMA((3,)),
                pltpu.SemaphoreType.DMA((2, cube)),
                pltpu.SemaphoreType.DMA((2, cube)),
                pltpu.SemaphoreType.DMA((3,)),
                pltpu.SemaphoreType.DMA((3,)),
                pltpu.SemaphoreType.DMA((14,)),
            ],
            compiler_params=pltpu.CompilerParams(
                collective_id=0, has_side_effects=True,
                vmem_limit_bytes=60 * 1024 * 1024),
        )(points, lengthscale[None, :], signal, noise, targets[None, :], probe_bits)
        return x + alpha * dx, r - alpha * dr

    both = ("row", "col")
    placed = (P(None, both), P(), P(), P(), P(both), P(None, both))
    return jax.shard_map(body, mesh=mesh, in_specs=placed, out_specs=(P(None, both),) * 2, check_vma=False)
```

```python
import functools
import math

import jax
import jax.numpy as jnp
from jax import lax
from jax.experimental import pallas as pl
from jax.experimental.pallas import tpu as pltpu
from jax.sharding import PartitionSpec as P

F32 = jnp.float32
BF16 = jnp.bfloat16
MESH = pl.DeviceIdType.MESH
LN2 = math.log(2.0)
SPREAD = math.sqrt(5.0) / LN2
LINEAR = 3.0 / LN2
CONSTANT = 3.0 / LN2**2
CHUNK = 1024


def pieces(x):
    first = x.astype(BF16).astype(F32)
    rest = x - first
    second = rest.astype(BF16).astype(F32)
    return first, second, (rest - second).astype(BF16).astype(F32)


def with_norms(x, before, after):
    parts = pieces(jnp.sum(x * x, axis=0, keepdims=True))
    row = lax.broadcasted_iota(jnp.int32, x.shape, 0)
    out = jnp.where((row >= after) & (row < after + 3), 1.0, 0.0)
    for i, part in enumerate(parts):
        out = jnp.where(row == before + i, part, out)
    return out


def left_operand(x):
    one, two, three = (-2.0 * p for p in pieces(x))
    return jnp.concatenate([one, one, two, two, one, three, with_norms(x, 0, 3), jnp.zeros_like(x)], axis=0)


def right_operand(x):
    one, two, three = pieces(x)
    return jnp.concatenate([one, two, one, two, three, one, with_norms(x, 3, 0), jnp.zeros_like(x)], axis=0)


def dot(a, b):
    return lax.dot_general(a, b, (((1,), (0,)), ((), ())), preferred_element_type=F32)


def flipped(v):
    return v + 1 - 2 * lax.rem(v, 2)


def turned(v):
    return lax.rem(v + 2 * lax.rem(v, 2) + 3, 4)


def kernel(rings, points, scales, signal, noise, targets, bits, out_x, out_r, out_dx, out_dr, out_alpha,
           points_here, scales_here, targets_here, bits_here, fetched, mine, mine_b, near, near_b, far, left, right, upper, lower, vectors, part, landed, gathered,
           met, summed, near_b_sem, near_sem, far_sem, land_sem, gather_sem, relay_sem, met_sem, summed_sem, sent):
    n = points_here.shape[1]
    cube = 2**rings
    pairs = cube // 2
    width = 2 * n
    depth = 2 * cube * n
    chunks = depth // CHUNK
    row, col = lax.axis_index("row"), lax.axis_index("col")
    core = lax.rem(row, 2)
    place = [row // 2]
    for i in range(rings - 1):
        place.append(lax.rem(col // 4 ** (rings - 2 - i), 4))

    def device(places, core):
        c = 0
        for v in places[1:]:
            c = 4 * c + v
        return {"row": 2 * places[0] + core, "col": c}

    def gather_partner(mask, other):
        return device([flipped(v) if mask >> i & 1 else v for i, v in enumerate(place)], 1 - core if other else core)

    def reduce_partner(mask):
        return device([v + lax.rem(mask // 2**i, 2) * (turned(v) - v) for i, v in enumerate(place)], core)

    def remote(src, dst, send, recv, to):
        return pltpu.make_async_remote_copy(
            src_ref=src, dst_ref=dst, send_sem=send, recv_sem=recv, device_id=to, device_id_type=MESH)

    def await_bytes(ref, sem):
        pltpu.make_async_copy(ref, ref, sem).wait()

    def each(lo, hi, fn):
        def step(i, carry):
            fn(i)
            return carry
        lax.fori_loop(lo, hi, step, 0)

    near_masks = sorted(range(1, cube), key=lambda m: (-bin(m).count("1"), m))
    slots = [(m, f) for m in near_masks for f in range(2)] + [(0, 1)]

    barrier = pltpu.get_barrier_semaphore()
    for m, f in slots:
        pl.semaphore_signal(barrier, inc=1, device_id=gather_partner(m, f), device_id_type=MESH)
    for m in near_masks:
        pl.semaphore_signal(barrier, inc=1, device_id=reduce_partner(m), device_id_type=MESH)
    local = [pltpu.make_async_copy(src, dst, fetched.at[i])
             for i, (src, dst) in enumerate(((points, points_here), (scales, scales_here), (targets, targets_here), (bits, bits_here)))]
    for copy in local:
        copy.start()
    for copy in local:
        copy.wait()
    diagonal = lax.broadcasted_iota(jnp.int32, (16, 16), 0) == lax.broadcasted_iota(jnp.int32, (16, 16), 1)
    scale = jnp.sum(jnp.where(diagonal, scales_here[...], 0.0), axis=1, keepdims=True)
    x = points_here[...] / scale * SPREAD
    mine[...] = x
    near[0] = x
    far[cube - 1] = x
    mine_b[0:1, :] = targets_here[...]
    mine_b[1:32, :] = 2.0 * bits_here[...].astype(F32) - 1.0
    near_b[0] = mine_b[...]

    def split_into(slot, d):
        at = pl.ds(slot * n if isinstance(slot, int) else pl.multiple_of(slot * n, n), n)
        high = d.astype(BF16)
        vectors[0:32, at] = high
        vectors[32:64, at] = (d - high.astype(F32)).astype(BF16)

    def place_left(i):
        left[i * n : i * n + n, :] = jnp.transpose(left_operand(near[i])).astype(BF16)

    def place_right(i):
        at = i % 2 * n if isinstance(i, int) else pl.multiple_of(lax.rem(i, 2) * n, n)
        right[i // 2, :, pl.ds(at, n)] = right_operand(far[i]).astype(BF16)

    vectors[64:128, :] = jnp.zeros((64, depth), BF16)
    split_into(0, near_b[0])
    place_left(0)
    place_right(cube - 1)
    pl.semaphore_wait(barrier, len(slots) + len(near_masks))

    def send_near(m, f):
        return remote(mine, near.at[f * cube + m], sent.at[0], near_sem.at[f * cube + m], gather_partner(m, f))

    for m in near_masks:
        remote(mine, far.at[cube - 1 - m], sent.at[1], far_sem.at[0], reduce_partner(m)).start()
    for m, f in slots:
        send_near(m, f).start()
    for m, f in slots:
        remote(mine_b, near_b.at[f * cube + m], sent.at[2], near_b_sem.at[0], gather_partner(m, f)).start()

    await_bytes(far.at[0 : cube - 1], far_sem.at[0])
    each(0, cube - 1, place_right)
    for m, f in reversed(slots):
        send_near(m, f).wait_recv()
        place_left(f * cube + m)

    def distances(p, c):
        return dot(left[pl.ds(pl.multiple_of(c * CHUNK, CHUNK), CHUNK), :], right[p])

    def evaluate(buffer, p, c):
        for at in range(0, CHUNK, 32):
            u = jnp.maximum(buffer[at : at + 32, :], 1e-30)
            q = u * lax.rsqrt(u)
            value = ((q + LINEAR) * q + CONSTANT) * jnp.exp2(-math.log2(CONSTANT) - q)
            high = value.astype(BF16)
            to = pl.ds(pl.multiple_of(c * CHUNK + at, 32), 32)
            upper[p, to, :] = high
            lower[p, to, :] = (value - upper[p, to, :].astype(F32)).astype(BF16)

    def product(p, at):
        v = vectors[:, at]
        both = dot(v, upper[p, at, :]) + dot(v, lower[p, at, :])
        return both[0:32] + both[32:64]

    def send_parts(k, p, total):
        for j in range(2):
            slot = 2 * p + j
            part[k, slot] = total[:, j * n : j * n + n]

            def send():
                remote(part.at[k, slot], landed.at[k, slot], sent.at[3 + k], land_sem.at[k],
                       reduce_partner(cube - 1 - slot)).start()

            if isinstance(p, int):
                if slot < cube - 1:
                    send()
            elif j == 0:
                send()
            else:
                pl.when(p < pairs - 1)(send)

    def step(t):
        for j in range(2):
            c = t * 2 + j
            evaluate(distances(c // chunks, lax.rem(c, chunks)), c // chunks, lax.rem(c, chunks))

    each(0, pairs * chunks // 2, step)
    await_bytes(near_b.at[1 : 2 * cube], near_b_sem.at[0])
    each(1, 2 * cube, lambda i: split_into(i, near_b[i]))
    each(0, pairs, lambda p: send_parts(0, p, product(p, pl.ds(0, depth))))

    def multiply(k):
        take_relayed(k - 1)
        pass_on(k - 1)
        def go(i):
            for j in range(2):
                send_parts(k, 2 * i + j, product(2 * i + j, pl.ds(0, depth)))

        each(0, pairs // 2, go)

    def at_home(k, v):
        await_bytes(landed.at[k], land_sem.at[k])
        total = part[k, cube - 1]
        for slot in range(cube - 1):
            total = total + landed[k, slot]
        return signal[0] * total + noise[0] * v

    def gather(k, w):
        gathered[k, 0] = w
        for m in near_masks:
            remote(gathered.at[k, 0], gathered.at[k, m], sent.at[6 + k], gather_sem.at[k, m], gather_partner(m, 0)).start()
        remote(gathered.at[k, 0], gathered.at[k, cube], sent.at[6 + k], relay_sem.at[k, 0], gather_partner(0, 1)).start()

    def relay(k, m):
        return remote(gathered.at[k, m], gathered.at[k, cube + m], sent.at[6 + k], relay_sem.at[k, m], gather_partner(0, 1))

    def take_gathered(k):
        split_into(0, gathered[k, 0])
        for m in reversed(near_masks):
            remote(gathered.at[k, 0], gathered.at[k, m], sent.at[6 + k], gather_sem.at[k, m], gather_partner(m, 0)).wait_recv()
            relay(k, m).start()
        for m in near_masks:
            split_into(m, gathered[k, m])

    def take_relayed(k):
        for m in [0, *reversed(near_masks)]:
            relay(k, m).wait_recv()
            split_into(cube + m, gathered[k, cube + m])

    lane = lax.broadcasted_iota(jnp.int32, (32, 128), 1)
    row_of = lax.broadcasted_iota(jnp.int32, (32, 128), 0)

    def tell(k, r, w):
        both = [jnp.sum(a, axis=1, keepdims=True) for a in (r * r, w * r)]
        met[k, 0:1] = sum(jnp.sum(jnp.where(lane == row_of + 32 * i, a, 0.0), axis=0, keepdims=True) for i, a in enumerate(both))
        for m, f in slots:
            at = f * cube + m
            remote(met.at[k, 0:1], met.at[k, at : at + 1], sent.at[8 + k], met_sem.at[k], gather_partner(m, f)).start()

    def pass_on(k):
        await_bytes(met.at[k, 1 : 2 * cube], met_sem.at[k])
        summed[k, cube - 1 : cube] = jnp.sum(met[k], axis=0, keepdims=True)
        for m in near_masks:
            at = cube - 1 - m
            remote(summed.at[k, cube - 1 : cube], summed.at[k, at : at + 1], sent.at[11 + k], summed_sem.at[k],
                   reduce_partner(m)).start()

    def hear(k):
        await_bytes(summed.at[k, 0 : cube - 1], summed_sem.at[k])
        total = jnp.sum(summed[k], axis=0, keepdims=True)
        return [jnp.sum(jnp.where(lane == row_of + 32 * i, total, 0.0), axis=1, keepdims=True) for i in range(2)]

    r = near_b[0]
    w = at_home(0, r)
    gather(0, w)
    tell(0, r, w)
    take_gathered(0)
    multiply(1)
    norm, curved = hear(0)
    alpha = norm / curved
    z = at_home(1, w)
    p, s = r, w
    r, w_next = r - alpha * s, w - alpha * z
    gather(1, w_next)
    tell(1, r, w_next)
    x = alpha * p
    take_gathered(1)
    multiply(2)
    w = w_next
    following, curved = hear(1)
    beta = following / norm
    norm, alpha = following, following / (curved - beta * following / alpha)
    p, s = r + beta * p, w + beta * s
    q = at_home(2, w)
    z = q + beta * z
    r, w = r - alpha * s, w - alpha * z
    tell(2, r, w)
    x = x + alpha * p
    pass_on(2)
    following, curved = hear(2)
    beta = following / norm
    alpha = following / (curved - beta * following / alpha)
    out_x[...] = x
    out_r[...] = r
    out_dx[...] = r + beta * p
    out_dr[...] = w + beta * s
    out_alpha[...] = jnp.broadcast_to(alpha, r.shape)

    await_bytes(near.at[1 : 2 * cube], sent.at[0])
    await_bytes(far.at[0 : cube - 1], sent.at[1])
    await_bytes(near_b.at[1 : 2 * cube], sent.at[2])
    for k in range(3):
        await_bytes(landed.at[k], sent.at[3 + k])
        await_bytes(met.at[k, 1 : 2 * cube], sent.at[8 + k])
        await_bytes(summed.at[k, 0 : cube - 1], sent.at[11 + k])
    for k in range(2):
        await_bytes(gathered.at[k, 1 : 2 * cube], sent.at[6 + k])


def solution(mesh):
    rings = {1: 1, 4: 2, 16: 3}[mesh.shape["col"]]
    cube = 2**rings

    def body(points, lengthscale, signal, noise, targets, probe_bits):
        n = points.shape[1]
        depth, width, block = 2 * cube * n, 2 * n, (32, n)
        vmem = pl.BlockSpec(memory_space=pltpu.VMEM)
        smem = pl.BlockSpec(memory_space=pltpu.SMEM)
        hbm = pl.BlockSpec(memory_space=pl.ANY)
        x, r, dx, dr, alpha = pl.pallas_call(
            functools.partial(kernel, rings),
            out_shape=(jax.ShapeDtypeStruct(block, F32),) * 5,
            in_specs=[hbm, hbm, smem, smem, hbm, hbm],
            out_specs=(vmem,) * 5,
            scratch_shapes=[
                pltpu.VMEM((16, n), F32),
                pltpu.VMEM((1, 16), F32),
                pltpu.VMEM((1, n), F32),
                pltpu.VMEM((31, n), jnp.int32),
                pltpu.SemaphoreType.DMA((4,)),
                pltpu.VMEM((16, n), F32),
                pltpu.VMEM(block, F32),
                pltpu.VMEM((2 * cube, 16, n), F32),
                pltpu.VMEM((2 * cube, *block), F32),
                pltpu.VMEM((cube, 16, n), F32),
                pltpu.VMEM((depth, 128), BF16),
                pltpu.VMEM((cube // 2, 128, width), BF16),
                pltpu.VMEM((cube // 2, depth, width), BF16),
                pltpu.VMEM((cube // 2, depth, width), BF16),
                pltpu.VMEM((128, depth), BF16),
                pltpu.VMEM((3, cube, *block), F32),
                pltpu.VMEM((3, cube - 1, *block), F32),
                pltpu.VMEM((2, 2 * cube, *block), F32),
                pltpu.VMEM((3, 2 * cube, 128), F32),
                pltpu.VMEM((3, cube, 128), F32),
                pltpu.SemaphoreType.DMA((1,)),
                pltpu.SemaphoreType.DMA((2 * cube,)),
                pltpu.SemaphoreType.DMA((1,)),
                pltpu.SemaphoreType.DMA((3,)),
                pltpu.SemaphoreType.DMA((2, cube)),
                pltpu.SemaphoreType.DMA((2, cube)),
                pltpu.SemaphoreType.DMA((3,)),
                pltpu.SemaphoreType.DMA((3,)),
                pltpu.SemaphoreType.DMA((14,)),
            ],
            compiler_params=pltpu.CompilerParams(
                collective_id=0, has_side_effects=True,
                vmem_limit_bytes=60 * 1024 * 1024),
        )(points, lengthscale[None, :], signal, noise, targets[None, :], probe_bits)
        return x + alpha * dx, r - alpha * dr

    both = ("row", "col")
    placed = (P(None, both), P(), P(), P(), P(both), P(None, both))
    return jax.shard_map(body, mesh=mesh, in_specs=placed, out_specs=(P(None, both),) * 2, check_vma=False)
```
